256 devices in a mesh: ctx: 32 (over z, x_hi, core), cand: 8 (over y, x_lo).
Axes of the slice: x: 4 (x_hi: 2, x_lo: 2; x = x_hi * 2 + x_lo), y: 4, z: 8, core: 2. Of those that a mesh axis runs over, the one named last changes fastest.
Arguments:
- queries: bfloat16 [2048, 1024], P(('cand', 'ctx')), may hold values from -256 to 256
- grad_out: bfloat16 [2048, 1024], P(('cand', 'ctx')), may hold values from -6 to 6
- prefix_keys: bfloat16 [32768, 128], P(('ctx', 'cand')), may hold values from -4 to 4
- prefix_values: bfloat16 [32768, 128], P(('ctx', 'cand')), may hold values from -6 to 6
- cand_keys: bfloat16 [2048, 128], P('cand'), may hold values from -6 to 6
- cand_values: bfloat16 [2048, 128], P('cand'), may hold values from -6 to 6
- lengths: int32 [8, 4], P('cand'), may hold values from 1 to 128, 256 in all within a row
- offsets: int32 [32], P('cand'), may hold values from 8192 to 32768
Outputs:
- grad_queries: bfloat16 [2048, 1024], P(('cand', 'ctx'))
- grad_keys: bfloat16 [32768, 128], P(('ctx', 'cand'))
- grad_values: bfloat16 [32768, 128], P(('ctx', 'cand'))
The draws below stay inside these ranges and needn't reach their ends.
Inputs may be any that keep to these rules, and one draw needn't show every extreme that they name: Each row of lengths sums to 256.
All inputs are finite; a program needn't handle non-finite values.
Results may differ from the reference program's by a relative error of at most 0.015.
Values may be sent and summed in bfloat16 or wider, within the bound.
A program may use at most 64 MiB of HBM per device.

```python
import math
import jax
import jax.numpy as jnp
import numpy as np
from jax import lax

HEADS = 8
HD = 128
C_BLK = 256
S_BLK = 4
PREFIX = 32768
CAND = 2048
SAMPLES = 32
N_CAND = 8


def base_keys(key):
    return jnp.clip(jax.random.normal(jax.random.fold_in(key, 11), (PREFIX, HD), jnp.float32), -4.0, 4.0)


def draw_prefix_keys(key, part):
    keys_base = base_keys(key)
    return keys_base.astype(jnp.bfloat16)


def draw_queries(key, part):
    drawn = jnp.clip(jax.random.normal(jax.random.fold_in(key, 23), (CAND, HEADS * HD), jnp.float32), -4.0, 4.0)
    return drawn.astype(jnp.bfloat16)


def set_ends(values, stream_key, low, largest):
    shape = values.shape
    place = [jax.random.randint(jax.random.fold_in(stream_key, axis), (), 0, shape[axis]) for axis in range(len(shape))]
    values = values.at[tuple(place)].set(low)
    longest = shape.index(max(shape))
    place[longest] = (place[longest] + 1) % shape[longest]
    return values.at[tuple(place)].set(largest)


def shard_levels(stream_key, extent, pieces, low, high):
    factor_of = 1.0
    for dim, parts in pieces:
        draws = jax.random.uniform(jax.random.fold_in(jax.random.fold_in(stream_key, 6), dim), (parts,), jnp.float32, low / len(pieces), high / len(pieces))
        factor_of = factor_of * jnp.repeat(jnp.exp(draws), extent[dim] // parts).reshape((-1,) + (1,) * (len(extent) - 1 - dim))
    return factor_of


def split_up(count, total, bound, lean):
    weights = [(1 << 20) // math.isqrt(standing ** lean) + 1 for standing in range(2, count + 1)]
    rest, given = total - bound - (count - 1), [1] * (count - 1)
    while rest > 0:
        movable = [i for i in range(count - 1) if given[i] < bound]
        whole, budget = sum([weights[i] for i in movable]), rest
        for i in movable:
            addition = min(bound - given[i], max(1, budget * weights[i] // whole), rest)
            given[i] = given[i] + addition
            rest = rest - addition
    return np.array([bound] + given)


def uneven_parts(rng, amount, total, bound, lean):
    if amount == 2:
        one = jax.random.randint(rng, (), max(1, total - bound), min(bound, total - 1) + 1)
        return jnp.stack([one, total - one])
    sizes = jnp.asarray(split_up(amount, total, bound, lean), jnp.int32)
    couples = (amount - 1) // 2
    giver, taker = sizes[1:1 + 2 * couples:2], sizes[2:2 + 2 * couples:2]
    slack = jnp.minimum(giver - 1, bound - taker)
    passed = jax.random.randint(jax.random.fold_in(rng, 1), (couples,), 0, 1 << 20) % (slack + 1)
    sizes = sizes.at[1:1 + 2 * couples:2].set(giver - passed).at[2:2 + 2 * couples:2].set(taker + passed)
    return sizes[jax.random.permutation(jax.random.fold_in(rng, 2), amount)]


def scatter_about(key, shape, spread, most, pieces=(), kind=jnp.bfloat16):
    result = spread * jax.random.normal(key, shape, jnp.float32)
    if pieces:
        result = result * shard_levels(key, shape, pieces, -0.22, 0.18)
    return jnp.clip(result, -most, most).astype(kind)


def setup_inputs(seed: int = 0) -> dict:
    splits = jax.random.split(jax.random.key(seed), 9)
    return {
        "queries": draw_queries(jax.random.fold_in(splits[8], 71), 0),
        "grad_out": scatter_about(splits[1], (CAND, HEADS * HD), 1.0, 6.0, ((0, 256),)),
        "prefix_keys": draw_prefix_keys(jax.random.fold_in(splits[8], 71), 0),
        "prefix_values": scatter_about(splits[3], (PREFIX, HD), 1.0, 6.0, ((0, 256),)),
        "cand_keys": scatter_about(splits[4], (CAND, HD), 1.0, 6.0, ((0, 8),)),
        "cand_values": scatter_about(splits[5], (CAND, HD), 1.0, 6.0, ((0, 8),)),
        "lengths": jax.vmap(lambda own: uneven_parts(own, S_BLK, C_BLK, C_BLK // 2, 2))(jax.random.split(splits[6], N_CAND)).reshape((N_CAND, S_BLK)).astype(jnp.int32),
        "offsets": set_ends(jax.random.randint(splits[7], (SAMPLES,), PREFIX // 4, PREFIX + 1), jax.random.fold_in(splits[7], 1), PREFIX // 4, PREFIX).astype(jnp.int32),
    }


NEG = -1e+30

def sample_rows(lengths, offsets):
    ends = jnp.cumsum(lengths, axis=1).astype(jnp.int32)
    local = jnp.arange(C_BLK, dtype=jnp.int32)
    segment = lax.optimization_barrier(jnp.sum((local[None, :, None] >= ends[:, None, :]).astype(jnp.int32), axis=2)).astype(jnp.int32)
    owner = (segment + (jnp.arange(N_CAND, dtype=jnp.int32) * S_BLK)[:, None]).astype(jnp.int32)
    limit = jnp.take(offsets, owner.reshape(-1)).reshape(N_CAND, C_BLK).astype(jnp.int32)
    return (segment, limit)

def reference(queries, grad_out, prefix_keys, prefix_values, cand_keys, cand_values, lengths, offsets):
    scaling = 1.0 / math.sqrt(HD)
    segment, limit = sample_rows(lengths, offsets)
    position = jnp.arange(PREFIX, dtype=jnp.int32)
    local = jnp.arange(C_BLK, dtype=jnp.int32)
    values_wide = prefix_values.astype(jnp.float32)
    query_heads = queries.reshape(N_CAND, C_BLK, HEADS, HD).transpose(0, 2, 1, 3)
    grad_heads = grad_out.reshape(N_CAND, C_BLK, HEADS, HD).transpose(0, 2, 1, 3)
    block_keys = cand_keys.reshape(N_CAND, C_BLK, HD)
    block_values = cand_values.reshape(N_CAND, C_BLK, HD)

    def one_block(carry, bundle):
        query_set, grad_set, own_keys, own_values, seg_block, limit_block = bundle
        seen = position[None, :] < limit_block[:, None]
        mine = (seg_block[:, None] == seg_block[None, :]) & (local[None, :] <= local[:, None])

        def one_head(pair):
            query, upstream = pair
            score_pre = jnp.dot(query, prefix_keys.T, preferred_element_type=jnp.float32) * scaling
            score_own = jnp.dot(query, own_keys.T, preferred_element_type=jnp.float32) * scaling
            highest = jnp.maximum(lax.optimization_barrier(jnp.max(jnp.where(seen, score_pre, NEG), axis=1)), lax.optimization_barrier(jnp.max(jnp.where(mine, score_own, NEG), axis=1)))
            exp_pre = jnp.where(seen, jnp.exp(score_pre - highest[:, None]), 0.0)
            exp_own = jnp.where(mine, jnp.exp(score_own - highest[:, None]), 0.0)
            totals = lax.optimization_barrier(jnp.sum(exp_pre, axis=1)) + lax.optimization_barrier(jnp.sum(exp_own, axis=1))
            prob_pre = exp_pre / totals[:, None]
            prob_own = exp_own / totals[:, None]
            output = jnp.dot(prob_pre, values_wide, precision=lax.Precision.HIGHEST, preferred_element_type=jnp.float32)
            output = output + jnp.dot(prob_own, own_values.astype(jnp.float32), precision=lax.Precision.HIGHEST, preferred_element_type=jnp.float32)
            delta = lax.optimization_barrier(jnp.sum(upstream.astype(jnp.float32) * output, axis=1))
            prod_pre = jnp.dot(upstream, prefix_values.T, preferred_element_type=jnp.float32)
            prod_own = jnp.dot(upstream, own_values.T, preferred_element_type=jnp.float32)
            slope_pre = (prob_pre * (prod_pre - delta[:, None])).astype(jnp.bfloat16)
            slope_own = (prob_own * (prod_own - delta[:, None])).astype(jnp.bfloat16)
            grad_query = scaling * (jnp.dot(slope_pre, prefix_keys, preferred_element_type=jnp.float32) + jnp.dot(slope_own, own_keys, preferred_element_type=jnp.float32))
            grad_key = scaling * jnp.dot(slope_pre.T, query, preferred_element_type=jnp.float32)
            grad_value = jnp.dot(prob_pre.astype(jnp.bfloat16).T, upstream, preferred_element_type=jnp.float32)
            return (grad_query, grad_key, grad_value)
        grad_query, grad_key, grad_value = lax.map(one_head, (query_set, grad_set))
        carry = (carry[0] + lax.optimization_barrier(jnp.sum(grad_key, axis=0)), carry[1] + lax.optimization_barrier(jnp.sum(grad_value, axis=0)))
        return (carry, grad_query)
    start = (jnp.zeros((PREFIX, HD), jnp.float32), jnp.zeros((PREFIX, HD), jnp.float32))
    (key_total, value_total), grad_query = lax.scan(one_block, start, (query_heads, grad_heads, block_keys, block_values, segment, limit))
    grad_queries = grad_query.transpose(0, 2, 1, 3).reshape(CAND, HEADS * HD).astype(jnp.bfloat16)
    return (grad_queries, key_total.astype(jnp.bfloat16), value_total.astype(jnp.bfloat16))
```

```python
import math

import jax
import jax.numpy as jnp
from jax import lax
from jax.experimental import pallas as pl
from jax.experimental.pallas import tpu as pltpu
from jax.sharding import Mesh
from jax.sharding import PartitionSpec as P

HEADS = 8
HD = 128
NX = NY = 4
NZ = 8
CHIPS = NX * NY
PEERS = 2 * CHIPS
TOK = 8
ROWS = TOK * HEADS
TILE = 4 * ROWS
TILES = PEERS * ROWS // TILE
KEYS = 128
GROUP = 2 * KEYS
GROUPS = NZ * KEYS // GROUP
SAMPLES = 4
AXES = ("z", "xh", "core", "y", "xl")
CAND = ("y", "xl")
CAND_CTX = ("y", "xl", "z", "xh", "core")
CTX_CAND = ("z", "xh", "core", "y", "xl")
MESH = pl.DeviceIdType.MESH
NEG = -1e30
SCALING = 1.0 / math.sqrt(HD)
SCORE = SCALING * math.log2(math.e)
PLACE = {0: 0, 1: 1, 7: 2, 2: 3, 6: 4, 3: 5, 5: 6, 4: 7}
BACK = {place: r for r, place in PLACE.items()}
F32 = jnp.float32
BF16 = jnp.bfloat16
NT = (((1,), (1,)), ((), ()))


def stacked(block):
    wide = block.astype(F32)
    return jnp.concatenate([wide[:, h * HD : (h + 1) * HD] for h in range(HEADS)], axis=0)


def kernel(
    q_ref, g_ref, pk_ref, pv_ref, ck_ref, cv_ref, len_ref, off_ref,
    gq_ref, gk_ref, gv_ref,
    qg, lim, kv, kt, e_buf, p_buf, sl_buf, mg, stat_out, stat_in, fin_out, fin,
    self_e, self_p, dq_out, dq_in, dq_self, part, rs_out, rs_in, rs_end,
    qg_send, qg_recv, lim_send, lim_recv, kv_send, kv_recv,
    st_send, st_recv, fin_send, fin_recv, dq_send, dq_recv,
    rs_send, rs_recv, end_recv,
):
    z, xh, core, y, xl = (lax.axis_index(a) for a in AXES)
    x = 2 * xh + xl
    chip = NY * x + y
    me = 2 * chip + core
    other = 1 - core
    mate = 2 * chip + other
    up = {"z": lax.rem(z + 1, NZ)}
    down = {"z": lax.rem(z + NZ - 1, NZ)}
    near = []
    for dx in range(NX):
        for dy in range(NY):
            if dx or dy:
                px, py = lax.rem(x + dx, NX), lax.rem(y + dy, NY)
                far = min(dx, NX - dx) + min(dy, NY - dy)
                place = {"xh": lax.div(px, 2), "xl": lax.rem(px, 2), "y": py}
                near.append((far, place, NY * px + py))
    near.sort(key=lambda item: item[0])
    sent = []

    def remote(src, dst, send_sem, recv_sem, device):
        return pltpu.make_async_remote_copy(
            src_ref=src, dst_ref=dst, send_sem=send_sem, recv_sem=recv_sem,
            device_id=device, device_id_type=MESH,
        )

    def send(*args):
        copy = remote(*args)
        copy.start()
        sent.append(copy)

    def arrived(dst, send_sem, recv_sem):
        remote(dst, dst, send_sem, recv_sem, {"core": other}).wait_recv()

    qg[me, 0] = stacked(q_ref[...]).astype(BF16)
    qg[me, 1] = stacked(g_ref[...]).astype(BF16)
    kv[0, 0] = pk_ref[...]
    kv[1, 0] = pv_ref[...]

    ends = [len_ref[0, 0]]
    for s in range(1, SAMPLES):
        ends.append(ends[-1] + len_ref[0, s])

    def sample_of(token):
        return sum((token >= end).astype(jnp.int32) for end in ends)

    lane = lax.broadcasted_iota(jnp.int32, (1, 2 * ROWS), 1)
    token = ((z * 2 + xh) * 2 + lax.div(lane, ROWS)) * TOK + lax.rem(lane, TOK)
    sample = sample_of(token)
    limit = jnp.zeros_like(sample)
    for s in range(SAMPLES):
        limit = jnp.where(sample == s, off_ref[s], limit)
    lim[chip] = limit

    barrier = pltpu.get_barrier_semaphore()
    for _, place, _ in near:
        for c in (core, other):
            pl.semaphore_signal(barrier, inc=1, device_id={**place, "core": c}, device_id_type=MESH)
    for place in ({"core": other}, up, down):
        pl.semaphore_signal(barrier, inc=1, device_id=place, device_id_type=MESH)
    pl.semaphore_wait(barrier, PEERS + 1)

    def ring(step):
        for kind in range(2):
            if step <= 4 - kind:
                src, dst = PLACE[step - 1], PLACE[step]
                source = (pk_ref, pv_ref)[kind] if step == 1 else kv.at[kind, src]
                send(source, kv.at[kind, dst], kv_send.at[kind, dst], kv_recv.at[kind, dst], up)
            if step <= 3 + kind:
                src, dst = PLACE[(9 - step) % 8], PLACE[8 - step]
                source = (pk_ref, pv_ref)[kind] if step == 1 else kv.at[kind, src]
                send(source, kv.at[kind, dst], kv_send.at[kind, dst], kv_recv.at[kind, dst], down)

    def ring_wait(step):
        for kind in range(2):
            for r in ([step] if step <= 4 - kind else []) + ([8 - step] if step <= 3 + kind else []):
                arrived(kv.at[kind, PLACE[r]], kv_send.at[kind, PLACE[r]], kv_recv.at[kind, PLACE[r]])

    def rows_wait(slot):
        arrived(qg.at[slot], qg_send.at[0], qg_recv.at[slot])

    def hand_over(slot, number):
        send(qg.at[slot], qg.at[slot], qg_send.at[number], qg_recv.at[slot], {"core": other})

    def plane_wait(far):
        for k, (dist, _, there) in enumerate(near):
            if dist == far:
                rows_wait(2 * there + core)
                hand_over(2 * there + core, CHIPS + k)

    ring(1)
    hand_over(me, 0)
    for k, (_, place, _) in reversed(list(enumerate(near))):
        send(qg.at[me], qg.at[me], qg_send.at[1 + k], qg_recv.at[me], place)
        send(lim.at[chip], lim.at[chip], lim_send.at[k], lim_recv.at[chip], place)

    ring_wait(1)
    ring(2)
    rows_wait(mate)

    own_q = qg[pl.ds(2 * chip, 2), 0].reshape(2 * ROWS, HD)
    own_g = qg[pl.ds(2 * chip, 2), 1].reshape(2 * ROWS, HD)
    block = ck_ref.shape[0]
    cand_token = lax.broadcasted_iota(jnp.int32, (block, 2 * ROWS), 0)
    allowed = (sample_of(cand_token) == sample) & (cand_token <= token)
    score = lax.dot_general(ck_ref[...], own_q, NT, preferred_element_type=F32) * SCORE
    score = jnp.where(allowed, score, NEG)
    own_high = jnp.max(score, axis=0, keepdims=True)
    expon = jnp.exp2(score - own_high)
    product = lax.dot_general(cv_ref[...], own_g, NT, preferred_element_type=F32)
    own_total = jnp.sum(expon, axis=0, keepdims=True)
    own_carry = jnp.sum(expon * product, axis=0, keepdims=True)
    self_e[...] = expon
    self_p[...] = product

    plane_wait(1)
    ring_wait(2)
    ring(3)
    plane_wait(2)
    ring_wait(3)
    ring(4)
    plane_wait(3)
    plane_wait(4)
    for k, (_, _, there) in enumerate(near):
        arrived(lim.at[there], lim_send.at[0], lim_recv.at[there])
    for k, (_, _, there) in enumerate(near):
        rows_wait(2 * there + other)
    ring_wait(4)

    def first_key(place):
        behind = lax.rem(z + NZ - BACK[place], NZ)
        return (((behind * 2 + xh) * 2 + core) * 8 + y * 2 + xl) * KEYS

    starts = [first_key(place) for place in range(NZ)]

    def first_pass(t, _):
        rows_q = qg[pl.ds(4 * t, 4), 0].reshape(TILE, HD)
        rows_g = qg[pl.ds(4 * t, 4), 1].reshape(TILE, HD)
        rows_limit = jnp.concatenate([lim[2 * t], lim[2 * t + 1]], axis=1)
        highs, totals, carries = [], [], []
        for g in range(GROUPS):
            keys = kv[0, 2 * g : 2 * g + 2].reshape(GROUP, HD)
            values = kv[1, 2 * g : 2 * g + 2].reshape(GROUP, HD)
            score = lax.dot_general(keys, rows_q, NT, preferred_element_type=F32) * SCORE
            index = lax.broadcasted_iota(jnp.int32, (KEYS, TILE), 0)
            seen = [index < rows_limit - starts[2 * g + i] for i in range(2)]
            score = jnp.concatenate(
                [jnp.where(seen[i], score[i * KEYS : (i + 1) * KEYS], NEG) for i in range(2)], axis=0
            )
            high = jnp.max(score, axis=0, keepdims=True)
            expon = jnp.exp2(score - high)
            product = lax.dot_general(values, rows_g, NT, preferred_element_type=F32)
            e_buf[t, g * GROUP : (g + 1) * GROUP] = expon
            p_buf[t, g * GROUP : (g + 1) * GROUP] = product
            highs.append(high)
            totals.append(jnp.sum(expon, axis=0, keepdims=True))
            carries.append(jnp.sum(expon * product, axis=0, keepdims=True))
        top = highs[0]
        for g in range(1, GROUPS):
            top = jnp.maximum(top, highs[g])
        total, carry = jnp.zeros_like(top), jnp.zeros_like(top)
        for g in range(GROUPS):
            weight = jnp.exp2(highs[g] - top)
            total += totals[g] * weight
            carry += carries[g] * weight
        mg[t] = jnp.concatenate(highs, axis=0)
        stats = jnp.concatenate([top, total, carry, top], axis=0)
        stat_out[2 * t] = stats[:, : 2 * ROWS]
        stat_out[2 * t + 1] = stats[:, 2 * ROWS :]
        return 0

    lax.fori_loop(0, TILES, first_pass, 0)

    for k, (_, place, there) in reversed(list(enumerate(near))):
        for i, c in enumerate((core, other)):
            send(
                stat_out.at[there], stat_in.at[me], st_send.at[2 * k + i], st_recv.at[me],
                {**place, "core": c},
            )
    send(stat_out.at[chip], stat_in.at[me], st_send.at[PEERS - 2], st_recv.at[me], {"core": other})
    stat_in[me] = stat_out[chip]
    for place in range(NZ):
        kt[:, place * KEYS : (place + 1) * KEYS] = kv[0, place].astype(F32).T.astype(BF16)
    arrived(stat_in.at[mate], st_send.at[0], st_recv.at[mate])
    for _, _, there in near:
        for c in (core, other):
            arrived(stat_in.at[2 * there + c], st_send.at[0], st_recv.at[2 * there + c])
    top = own_high
    for i in range(PEERS):
        top = jnp.maximum(top, stat_in[i][0:1])
    weight = jnp.exp2(own_high - top)
    total, carry = own_total * weight, own_carry * weight
    for i in range(PEERS):
        stats = stat_in[i]
        weight = jnp.exp2(stats[0:1] - top)
        total += stats[1:2] * weight
        carry += stats[2:3] * weight
    inverse = 1.0 / total
    delta = carry * inverse
    final = jnp.concatenate([top, inverse, delta, top], axis=0)
    fin_out[...] = final
    fin[chip] = final
    for k, (_, place, _) in reversed(list(enumerate(near))):
        send(fin_out, fin.at[chip], fin_send.at[k], fin_recv.at[chip], place)

    self_probs = self_e[...] * (jnp.exp2(own_high - top) * inverse)
    self_slopes = (self_probs * (self_p[...] - delta)).astype(BF16)
    self_keys = ck_ref[...].astype(F32).T.astype(BF16)
    dq_self[...] = (jnp.dot(self_keys, self_slopes, preferred_element_type=F32) * SCALING).T

    for _, _, there in near:
        arrived(fin.at[there], fin_send.at[0], fin_recv.at[there])

    def second_pass(place, _):
        g = lax.div(place, 2)
        grad_k = jnp.zeros((KEYS, HD), F32)
        grad_v = jnp.zeros((KEYS, HD), F32)
        for t in range(TILES):
            final = jnp.concatenate([fin[2 * t], fin[2 * t + 1]], axis=1)
            weight = jnp.exp2(mg[t, pl.ds(g, 1)] - final[0:1]) * final[1:2]
            at = pl.ds(pl.multiple_of(place * KEYS, KEYS), KEYS)
            probs = e_buf[t, at] * weight
            slopes = (probs * (p_buf[t, at] - final[2:3])).astype(BF16)
            sl_buf[t, at] = slopes
            rows_q = qg[4 * t : 4 * t + 4, 0].reshape(TILE, HD)
            rows_g = qg[4 * t : 4 * t + 4, 1].reshape(TILE, HD)
            grad_v += jnp.dot(probs.astype(BF16), rows_g, preferred_element_type=F32)
            grad_k += jnp.dot(slopes, rows_q, preferred_element_type=F32)
        part[place, 0] = grad_k * SCALING
        part[place, 1] = grad_v
        return 0

    def pass_on(back, kind, first):
        place = PLACE[back]
        total = part[place, kind]
        if not first:
            arrived(rs_in.at[kind, place], rs_send.at[kind, place], rs_recv.at[kind, place])
            total = total + rs_in[kind, place].astype(F32)
        rs_out[kind, place] = total.astype(BF16)
        going_down = back < 4 or (back == 4 and kind == 0)
        nearer = back - 1 if going_down else (back + 1) % 8
        way = 0 if going_down else 1
        if nearer:
            dst, sem = rs_in.at[kind, PLACE[nearer]], rs_recv.at[kind, PLACE[nearer]]
        else:
            dst, sem = rs_end.at[kind, way], end_recv.at[kind, way]
        send(rs_out.at[kind, place], dst, rs_send.at[kind, place], sem, down if going_down else up)

    second_pass(7, 0)
    pass_on(4, 0, True)
    pass_on(4, 1, True)
    lax.fori_loop(0, 4, lambda i, c: second_pass(6 - i, c), 0)
    pass_on(5, 0, True)
    pass_on(3, 1, True)
    pass_on(3, 0, False)
    pass_on(5, 1, False)
    lax.fori_loop(0, 3, lambda i, c: second_pass(2 - i, c), 0)
    for back in (2, 6):
        for kind in range(2):
            pass_on(back, kind, False)

    def query_pass(t, _):
        grads = jnp.dot(kt[...], sl_buf[t], preferred_element_type=F32) * SCALING
        dq_out[pl.ds(4 * t, 4)] = grads.T.astype(BF16).reshape(4, ROWS, HD)
        return 0

    lax.fori_loop(0, TILES, query_pass, 0)
    for k, (_, place, there) in reversed(list(enumerate(near))):
        for i, c in enumerate((core, other)):
            send(
                dq_out.at[2 * there + c], dq_in.at[me], dq_send.at[2 * k + i], dq_recv.at[me],
                {**place, "core": c},
            )
    send(dq_out.at[mate], dq_in.at[me], dq_send.at[PEERS - 2], dq_recv.at[me], {"core": other})
    dq_in[me] = dq_out[me]
    for back in (1, 7):
        for kind in range(2):
            pass_on(back, kind, False)
    arrived(dq_in.at[mate], dq_send.at[0], dq_recv.at[mate])
    for _, _, there in near:
        for c in (core, other):
            arrived(dq_in.at[2 * there + c], dq_send.at[0], dq_recv.at[2 * there + c])
    grads = dq_self[pl.ds(pl.multiple_of(core * ROWS, ROWS), ROWS)]
    for i in range(PEERS):
        grads += dq_in[i].astype(F32)
    gq_ref[...] = jnp.concatenate(
        [grads[h * TOK : (h + 1) * TOK] for h in range(HEADS)], axis=1
    ).astype(BF16)
    for kind, out in enumerate((gk_ref, gv_ref)):
        total = part[0, kind]
        for way in range(2):
            arrived(rs_end.at[kind, way], rs_send.at[kind, 0], end_recv.at[kind, way])
            total = total + rs_end[kind, way].astype(F32)
        out[...] = total.astype(BF16)
    for copy in sent:
        copy.wait_send()


def body(queries, grad_out, prefix_keys, prefix_values, cand_keys, cand_values, lengths, offsets):
    vmem = pl.BlockSpec(memory_space=pltpu.VMEM)
    smem = pl.BlockSpec(memory_space=pltpu.SMEM)
    keys = NZ * KEYS
    block = cand_keys.shape[0]
    sem = pltpu.SemaphoreType.DMA
    return pl.pallas_call(
        kernel,
        out_shape=(
            jax.ShapeDtypeStruct(queries.shape, BF16),
            jax.ShapeDtypeStruct(prefix_keys.shape, BF16),
            jax.ShapeDtypeStruct(prefix_values.shape, BF16),
        ),
        in_specs=[vmem] * 6 + [smem] * 2,
        out_specs=(vmem,) * 3,
        scratch_shapes=[
            pltpu.VMEM((PEERS, 2, ROWS, HD), BF16),
            pltpu.VMEM((CHIPS, 1, 2 * ROWS), jnp.int32),
            pltpu.VMEM((2, NZ, KEYS, HD), BF16),
            pltpu.VMEM((HD, keys), BF16),
            pltpu.VMEM((TILES, keys, TILE), F32),
            pltpu.VMEM((TILES, keys, TILE), F32),
            pltpu.VMEM((TILES, keys, TILE), BF16),
            pltpu.VMEM((TILES, GROUPS, TILE), F32),
            pltpu.VMEM((CHIPS, 4, 2 * ROWS), F32),
            pltpu.VMEM((PEERS, 4, 2 * ROWS), F32),
            pltpu.VMEM((4, 2 * ROWS), F32),
            pltpu.VMEM((CHIPS, 4, 2 * ROWS), F32),
            pltpu.VMEM((block, 2 * ROWS), F32),
            pltpu.VMEM((block, 2 * ROWS), F32),
            pltpu.VMEM((PEERS, ROWS, HD), BF16),
            pltpu.VMEM((PEERS, ROWS, HD), BF16),
            pltpu.VMEM((2 * ROWS, HD), F32),
            pltpu.VMEM((NZ, 2, KEYS, HD), F32),
            pltpu.VMEM((2, NZ, KEYS, HD), BF16),
            pltpu.VMEM((2, NZ, KEYS, HD), BF16),
            pltpu.VMEM((2, 2, KEYS, HD), BF16),
            sem((PEERS - 1,)),
            sem((PEERS,)),
            sem((CHIPS - 1,)),
            sem((CHIPS,)),
            sem((2, NZ)),
            sem((2, NZ)),
            sem((PEERS - 1,)),
            sem((PEERS,)),
            sem((CHIPS - 1,)),
            sem((CHIPS,)),
            sem((PEERS - 1,)),
            sem((PEERS,)),
            sem((2, NZ)),
            sem((2, NZ)),
            sem((2, 2)),
        ],
        compiler_params=pltpu.CompilerParams(
            collective_id=0, has_side_effects=True, vmem_limit_bytes=56 * 1024 * 1024
        ),
        name="attention_grads",
    )(queries, grad_out, prefix_keys, prefix_values, cand_keys, cand_values, lengths, offsets)


def solution(mesh):
    torus = Mesh(mesh.devices.reshape(NZ, 2, 2, NY, 2), AXES)
    in_specs = (
        P(CAND_CTX, None),
        P(CAND_CTX, None),
        P(CTX_CAND, None),
        P(CTX_CAND, None),
        P(CAND, None),
        P(CAND, None),
        P(CAND, None),
        P(CAND),
    )
    out_specs = (P(CAND_CTX, None), P(CTX_CAND, None), P(CTX_CAND, None))
    return jax.shard_map(body, mesh=torus, in_specs=in_specs, out_specs=out_specs, check_vma=False)
```

```python
import math

import jax
import jax.numpy as jnp
from jax import lax
from jax.experimental import pallas as pl
from jax.experimental.pallas import tpu as pltpu
from jax.sharding import Mesh
from jax.sharding import PartitionSpec as P

HEADS = 8
HD = 128
NX = NY = 4
NZ = 8
CHIPS = NX * NY
PEERS = 2 * CHIPS
TOK = 8
ROWS = TOK * HEADS
TILE = 4 * ROWS
TILES = PEERS * ROWS // TILE
KEYS = 128
GROUPS = ((0, 2), (2, 5), (5, 8))
SAMPLES = 4
AXES = ("z", "xh", "core", "y", "xl")
CAND = ("y", "xl")
CAND_CTX = ("y", "xl", "z", "xh", "core")
CTX_CAND = ("z", "xh", "core", "y", "xl")
MESH = pl.DeviceIdType.MESH
NEG = -1e30
SCALING = 1.0 / math.sqrt(HD)
SCORE = SCALING * math.log2(math.e)
PLACE = {0: 0, 1: 1, 7: 2, 2: 3, 6: 4, 3: 5, 5: 6, 4: 7}
BACK = {place: r for r, place in PLACE.items()}
OFFSETS = sorted(
    ((dx, dy) for dx in range(NX) for dy in range(NY)),
    key=lambda o: min(o[0], NX - o[0]) + min(o[1], NY - o[1]),
)
FAR = [min(dx, NX - dx) + min(dy, NY - dy) for dx, dy in OFFSETS]
SEEN = [OFFSETS.index(((NX - dx) % NX, (NY - dy) % NY)) for dx, dy in OFFSETS]
F32 = jnp.float32
BF16 = jnp.bfloat16
NT = (((1,), (1,)), ((), ()))


def stacked(block):
    wide = block.astype(F32)
    return jnp.concatenate([wide[:, h * HD : (h + 1) * HD] for h in range(HEADS)], axis=0)


def kernel(
    q_ref, g_ref, pk_ref, pv_ref, ck_ref, cv_ref, len_ref, off_ref,
    gq_ref, gk_ref, gv_ref,
    qg, lim, kv, kt, e_buf, p_buf, mg, tot, car, loc, ab, stat_out, stat_in, fin_out, fin,
    self_e, self_p, dq_out, dq_mate, dq_sum, dq_in, dq_self, part, rs_out, rs_near, rs_far, rs_end,
    qg_send, qg_recv, lim_send, lim_recv, kv_send, kv_recv,
    st_send, st_recv, fin_send, fin_recv, mate_send, mate_recv, dq_send, dq_recv,
    rs_send, near_recv, far_recv, end_recv,
):
    z, xh, core, y, xl = (lax.axis_index(a) for a in AXES)
    x = 2 * xh + xl
    other = 1 - core
    mate = {"core": other}
    up, up2, down2, down = ({"z": lax.rem(z + d, NZ)} for d in (1, 2, NZ - 2, NZ - 1))
    chips = []
    for dx, dy in OFFSETS:
        px, py = lax.rem(x + dx, NX), lax.rem(y + dy, NY)
        chips.append({"xh": lax.div(px, 2), "xl": lax.rem(px, 2), "y": py})
    nearest = list(range(1, CHIPS))
    farthest = nearest[::-1]
    sent = []

    def remote(src, dst, send_sem, recv_sem, device):
        return pltpu.make_async_remote_copy(
            src_ref=src, dst_ref=dst, send_sem=send_sem, recv_sem=recv_sem,
            device_id=device, device_id_type=MESH,
        )

    def send(*args):
        copy = remote(*args)
        copy.start()
        sent.append(copy)

    def arrived(dst, send_sem, recv_sem):
        remote(dst, dst, send_sem, recv_sem, mate).wait_recv()

    qg[core, 0] = stacked(q_ref[...]).astype(BF16)
    qg[core, 1] = stacked(g_ref[...]).astype(BF16)
    kv[0, 0] = pk_ref[...]
    kv[1, 0] = pv_ref[...]

    ends = [len_ref[0, 0]]
    for s in range(1, SAMPLES):
        ends.append(ends[-1] + len_ref[0, s])

    def sample_of(token):
        return sum((token >= end).astype(jnp.int32) for end in ends)

    lane = lax.broadcasted_iota(jnp.int32, (1, 2 * ROWS), 1)
    token = ((z * 2 + xh) * 2 + lax.div(lane, ROWS)) * TOK + lax.rem(lane, TOK)
    sample = sample_of(token)
    limit = jnp.zeros_like(sample)
    for s in range(SAMPLES):
        limit = jnp.where(sample == s, off_ref[s], limit)
    lim[0] = limit

    barrier = pltpu.get_barrier_semaphore()
    for r in nearest:
        for c in (core, other):
            pl.semaphore_signal(
                barrier, inc=1, device_id={**chips[r], "core": c}, device_id_type=MESH
            )
    for device in (mate, up, down, up2, down2):
        pl.semaphore_signal(barrier, inc=1, device_id=device, device_id_type=MESH)
    pl.semaphore_wait(barrier, PEERS + 3)

    def kv_to(kind, back, new_back, device):
        src = (pk_ref, pv_ref)[kind] if back == 0 else kv.at[kind, PLACE[back]]
        at = PLACE[new_back]
        send(src, kv.at[kind, at], kv_send.at[kind, at], kv_recv.at[kind, at], device)

    def kv_wait(kind, back):
        at = PLACE[back]
        arrived(kv.at[kind, at], kv_send.at[kind, at], kv_recv.at[kind, at])

    def rows_wait(slot):
        arrived(qg.at[slot], qg_send.at[0], qg_recv.at[slot])

    def hand_over(r):
        slot = 2 * r + core
        send(qg.at[slot], qg.at[slot], qg_send.at[r], qg_recv.at[slot], mate)

    def plane_wait(far):
        for r in nearest:
            if FAR[r] == far:
                rows_wait(2 * r + core)
                hand_over(r)

    for kind in range(2):
        kv_to(kind, 0, 2, up2)
        kv_to(kind, 0, 6, down2)
    hand_over(0)
    for r in farthest:
        slot = 2 * SEEN[r] + core
        send(qg.at[core], qg.at[slot], qg_send.at[CHIPS - 1 + r], qg_recv.at[slot], chips[r])
    for kind in range(2):
        kv_to(kind, 0, 1, up)
        kv_to(kind, 0, 7, down)
    for r in farthest:
        send(lim.at[0], lim.at[SEEN[r]], lim_send.at[r], lim_recv.at[SEEN[r]], chips[r])

    rows_wait(other)
    own_q = qg[0:2, 0].reshape(2 * ROWS, HD)
    own_g = qg[0:2, 1].reshape(2 * ROWS, HD)
    block = ck_ref.shape[0]
    cand_token = lax.broadcasted_iota(jnp.int32, (block, 2 * ROWS), 0)
    allowed = (sample_of(cand_token) == sample) & (cand_token <= token)
    score = lax.dot_general(ck_ref[...], own_q, NT, preferred_element_type=F32) * SCORE
    score = jnp.where(allowed, score, NEG)
    own_high = jnp.max(score, axis=0, keepdims=True)
    expon = jnp.exp2(score - own_high)
    product = lax.dot_general(cv_ref[...], own_g, NT, preferred_element_type=F32)
    own_total = jnp.sum(expon, axis=0, keepdims=True)
    own_carry = jnp.sum(expon * product, axis=0, keepdims=True)
    self_e[...] = expon
    self_p[...] = product

    def first_key(place):
        behind = lax.rem(z + NZ - BACK[place], NZ)
        return (((behind * 2 + xh) * 2 + core) * 8 + y * 2 + xl) * KEYS

    starts = [first_key(place) for place in range(NZ)]

    def first_pass(t, groups):
        rows_q = qg[pl.ds(4 * t, 4), 0].reshape(TILE, HD)
        rows_g = qg[pl.ds(4 * t, 4), 1].reshape(TILE, HD)
        rows_limit = jnp.concatenate([lim[2 * t], lim[2 * t + 1]], axis=1)
        for g in groups:
            low, high = GROUPS[g]
            count = (high - low) * KEYS
            keys = kv[0, low:high].reshape(count, HD)
            values = kv[1, low:high].reshape(count, HD)
            score = lax.dot_general(keys, rows_q, NT, preferred_element_type=F32) * SCORE
            index = lax.broadcasted_iota(jnp.int32, (KEYS, TILE), 0)
            masked = []
            for i, place in enumerate(range(low, high)):
                seen = index < rows_limit - starts[place]
                masked.append(jnp.where(seen, score[i * KEYS : (i + 1) * KEYS], NEG))
            score = jnp.concatenate(masked, axis=0)
            top = jnp.max(score, axis=0, keepdims=True)
            expon = jnp.exp2(score - top)
            product = lax.dot_general(values, rows_g, NT, preferred_element_type=F32)
            e_buf[t, low * KEYS : high * KEYS] = expon
            p_buf[t, low * KEYS : high * KEYS] = product
            mg[t, g : g + 1] = top
            tot[t, g : g + 1] = jnp.sum(expon, axis=0, keepdims=True)
            car[t, g : g + 1] = jnp.sum(expon * product, axis=0, keepdims=True)

    def run_first_pass(start, stop, groups):
        def step(t, carry):
            first_pass(t, groups)
            return carry

        lax.fori_loop(start, stop, step, 0)

    def close_rows(t, carry):
        highs = mg[t]
        top = jnp.max(highs, axis=0, keepdims=True)
        weight = jnp.exp2(highs - top)
        total = jnp.sum(tot[t] * weight, axis=0, keepdims=True)
        carried = jnp.sum(car[t] * weight, axis=0, keepdims=True)
        loc[t] = jnp.concatenate([top, carried / total], axis=0)
        stats = jnp.concatenate([top, total, carried, top], axis=0)
        stat_out[2 * t] = stats[:, : 2 * ROWS]
        stat_out[2 * t + 1] = stats[:, 2 * ROWS :]
        return carry

    def tile_wait(tiles):
        for t in tiles:
            for r in (2 * t, 2 * t + 1):
                if r:
                    rows_wait(2 * r + other)
                    arrived(lim.at[r], lim_send.at[1], lim_recv.at[r])

    plane_wait(1)
    kv_wait(0, 2)
    kv_to(0, 2, 4, up2)
    kv_to(0, 2, 3, up)
    kv_wait(0, 6)
    kv_to(0, 6, 5, down)
    kv_wait(1, 6)
    kv_to(1, 6, 4, down2)
    kv_to(1, 6, 5, down)
    kv_wait(1, 2)
    kv_to(1, 2, 3, up)
    plane_wait(2)
    for kind in range(2):
        for back in (1, 7):
            kv_wait(kind, back)
    tile_wait((0, 1))
    run_first_pass(0, 2, (0, 1))
    plane_wait(3)
    plane_wait(4)
    tile_wait((2, 3, 4))
    run_first_pass(2, 5, (0, 1))
    for kind in range(2):
        for back in (3, 5, 4):
            kv_wait(kind, back)
    run_first_pass(0, 5, (2,))
    tile_wait((5, 6, 7))
    run_first_pass(5, TILES, (0, 1, 2))
    lax.fori_loop(0, TILES, close_rows, 0)

    for r in farthest:
        for i, c in enumerate((core, other)):
            slot = 2 * SEEN[r] + core
            send(
                stat_out.at[r], stat_in.at[slot], st_send.at[2 * r + i], st_recv.at[slot],
                {**chips[r], "core": c},
            )
    send(stat_out.at[0], stat_in.at[core], st_send.at[0], st_recv.at[core], mate)
    stat_in[core] = stat_out[0]

    for place in range(NZ):
        kt[:, place * KEYS : (place + 1) * KEYS] = kv[0, place].astype(F32).T.astype(BF16)

    def query_products(t, carry):
        top, delta = loc[t, 0:1], loc[t, 1:2]
        expons, slopes = [], []
        for g, (low, high) in enumerate(GROUPS):
            weight = jnp.exp2(mg[t, g : g + 1] - top)
            expon = e_buf[t, low * KEYS : high * KEYS] * weight
            expons.append(expon.astype(BF16))
            slopes.append((expon * (p_buf[t, low * KEYS : high * KEYS] - delta)).astype(BF16))
        for i, right in enumerate((slopes, expons)):
            ab[t, i] = jnp.dot(kt[...], jnp.concatenate(right, axis=0), preferred_element_type=F32)
        return carry

    lax.fori_loop(0, TILES, query_products, 0)

    arrived(stat_in.at[other], st_send.at[0], st_recv.at[other])
    for r in nearest:
        for c in (core, other):
            arrived(stat_in.at[2 * r + c], st_send.at[0], st_recv.at[2 * r + c])
    top = own_high
    for i in range(PEERS):
        top = jnp.maximum(top, stat_in[i][0:1])
    weight = jnp.exp2(own_high - top)
    total, carried = own_total * weight, own_carry * weight
    for i in range(PEERS):
        stats = stat_in[i]
        weight = jnp.exp2(stats[0:1] - top)
        total += stats[1:2] * weight
        carried += stats[2:3] * weight
    inverse = 1.0 / total
    delta = carried * inverse
    final = jnp.concatenate([top, inverse, delta, top], axis=0)
    fin_out[...] = final
    fin[0] = final
    for r in farthest:
        send(fin_out, fin.at[SEEN[r]], fin_send.at[r], fin_recv.at[SEEN[r]], chips[r])

    self_probs = self_e[...] * (jnp.exp2(own_high - top) * inverse)
    self_slopes = (self_probs * (self_p[...] - delta)).astype(BF16)
    self_keys = ck_ref[...].astype(F32).T.astype(BF16)
    dq_self[...] = (jnp.dot(self_keys, self_slopes, preferred_element_type=F32) * SCALING).T

    for r in nearest:
        arrived(fin.at[r], fin_send.at[1], fin_recv.at[r])

    def close_weights(t, carry):
        final = jnp.concatenate([fin[2 * t], fin[2 * t + 1]], axis=1)
        mg[t] = jnp.exp2(mg[t] - final[0:1]) * final[1:2]
        return carry

    lax.fori_loop(0, TILES, close_weights, 0)

    def second_pass(place, carry):
        g = lax.div(place + 1, 3)
        grad_k = jnp.zeros((KEYS, HD), F32)
        grad_v = jnp.zeros((KEYS, HD), F32)
        for t in range(TILES):
            delta = jnp.concatenate([fin[2 * t, 2:3], fin[2 * t + 1, 2:3]], axis=1)
            at = pl.ds(pl.multiple_of(place * KEYS, KEYS), KEYS)
            probs = e_buf[t, at] * mg[t, pl.ds(g, 1)]
            slopes = (probs * (p_buf[t, at] - delta)).astype(BF16)
            rows_q = qg[4 * t : 4 * t + 4, 0].reshape(TILE, HD)
            rows_g = qg[4 * t : 4 * t + 4, 1].reshape(TILE, HD)
            grad_v += jnp.dot(probs.astype(BF16), rows_g, preferred_element_type=F32)
            grad_k += jnp.dot(slopes, rows_q, preferred_element_type=F32)
        part[place, 0] = grad_k * SCALING
        part[place, 1] = grad_v
        return carry

    def pass_on(kind, back, dst, sem, device, *more):
        at = PLACE[back]
        total = part[at, kind]
        for ref in more:
            total = total + ref[...].astype(F32)
        rs_out[kind, at] = total.astype(BF16)
        send(rs_out.at[kind, at], dst, rs_send.at[kind, at], sem, device)

    lax.fori_loop(0, 3, lambda i, c: second_pass(7 - i, c), 0)
    pass_on(0, 4, rs_far.at[0], far_recv.at[0], down2)
    pass_on(1, 4, rs_far.at[1], far_recv.at[1], up2)
    for kind in range(2):
        pass_on(kind, 3, rs_near.at[kind, 0], near_recv.at[kind, 0], down)
        pass_on(kind, 5, rs_near.at[kind, 1], near_recv.at[kind, 1], up)

    def query_pass(t, carry):
        final = jnp.concatenate([fin[2 * t], fin[2 * t + 1]], axis=1)
        weight = jnp.exp2(loc[t, 0:1] - final[0:1]) * final[1:2] * SCALING
        grads = (ab[t, 0] - ab[t, 1] * (final[2:3] - loc[t, 1:2])) * weight
        rows = grads.T.astype(BF16)
        for i in range(2):
            for c in range(2):
                at = (2 * i + c) * ROWS
                dq_out[c, 2 * t + i] = rows[at : at + ROWS]
        return carry

    lax.fori_loop(0, TILES, query_pass, 0)
    send(dq_out.at[other], dq_mate, mate_send, mate_recv, mate)
    lax.fori_loop(0, 3, lambda i, c: second_pass(4 - i, c), 0)
    arrived(dq_mate, mate_send, mate_recv)

    def add_mate(r, carry):
        dq_sum[r] = (dq_out[core, r].astype(F32) + dq_mate[r].astype(F32)).astype(BF16)
        return carry

    lax.fori_loop(0, CHIPS, add_mate, 0)
    for r in farthest:
        send(dq_sum.at[r], dq_in.at[SEEN[r]], dq_send.at[r], dq_recv.at[SEEN[r]], chips[r])
    lax.fori_loop(0, 2, lambda i, c: second_pass(1 - i, c), 0)
    for kind in range(2):
        pass_on(kind, 7, rs_end.at[kind, 2], end_recv.at[kind, 2], up)
        pass_on(kind, 1, rs_end.at[kind, 0], end_recv.at[kind, 0], down)

    def two_on(kind, way):
        arrived(rs_near.at[kind, way], rs_send.at[kind, 0], near_recv.at[kind, way])
        more = [rs_near.at[kind, way]]
        if kind == way:
            arrived(rs_far.at[way], rs_send.at[kind, 0], far_recv.at[way])
            more.append(rs_far.at[way])
        slot = 1 + 2 * way
        device = (down2, up2)[way]
        pass_on(
            kind, (2, 6)[way], rs_end.at[kind, slot], end_recv.at[kind, slot], device, *more
        )

    for kind, way in ((0, 0), (1, 1), (1, 0), (0, 1)):
        two_on(kind, way)

    grads = dq_self[pl.ds(pl.multiple_of(core * ROWS, ROWS), ROWS)] + dq_sum[0].astype(F32)
    for r in nearest:
        arrived(dq_in.at[r], dq_send.at[1], dq_recv.at[r])
        grads += dq_in[r].astype(F32)
    gq_ref[...] = jnp.concatenate(
        [grads[h * TOK : (h + 1) * TOK] for h in range(HEADS)], axis=1
    ).astype(BF16)
    for kind, out in enumerate((gk_ref, gv_ref)):
        total = part[0, kind]
        for way in (0, 2, 1, 3):
            arrived(rs_end.at[kind, way], rs_send.at[kind, 0], end_recv.at[kind, way])
            total = total + rs_end[kind, way].astype(F32)
        out[...] = total.astype(BF16)
    for copy in sent:
        copy.wait_send()


def body(queries, grad_out, prefix_keys, prefix_values, cand_keys, cand_values, lengths, offsets):
    vmem = pl.BlockSpec(memory_space=pltpu.VMEM)
    smem = pl.BlockSpec(memory_space=pltpu.SMEM)
    keys = NZ * KEYS
    block = cand_keys.shape[0]
    sem = pltpu.SemaphoreType.DMA
    return pl.pallas_call(
        kernel,
        out_shape=(
            jax.ShapeDtypeStruct(queries.shape, BF16),
            jax.ShapeDtypeStruct(prefix_keys.shape, BF16),
            jax.ShapeDtypeStruct(prefix_values.shape, BF16),
        ),
        in_specs=[vmem] * 6 + [smem] * 2,
        out_specs=(vmem,) * 3,
        scratch_shapes=[
            pltpu.VMEM((PEERS, 2, ROWS, HD), BF16),
            pltpu.VMEM((CHIPS, 1, 2 * ROWS), jnp.int32),
            pltpu.VMEM((2, NZ, KEYS, HD), BF16),
            pltpu.VMEM((HD, keys), BF16),
            pltpu.VMEM((TILES, keys, TILE), F32),
            pltpu.VMEM((TILES, keys, TILE), F32),
            pltpu.VMEM((TILES, len(GROUPS), TILE), F32),
            pltpu.VMEM((TILES, len(GROUPS), TILE), F32),
            pltpu.VMEM((TILES, len(GROUPS), TILE), F32),
            pltpu.VMEM((TILES, 2, TILE), F32),
            pltpu.VMEM((TILES, 2, HD, TILE), F32),
            pltpu.VMEM((CHIPS, 4, 2 * ROWS), F32),
            pltpu.VMEM((PEERS, 4, 2 * ROWS), F32),
            pltpu.VMEM((4, 2 * ROWS), F32),
            pltpu.VMEM((CHIPS, 4, 2 * ROWS), F32),
            pltpu.VMEM((block, 2 * ROWS), F32),
            pltpu.VMEM((block, 2 * ROWS), F32),
            pltpu.VMEM((2, CHIPS, ROWS, HD), BF16),
            pltpu.VMEM((CHIPS, ROWS, HD), BF16),
            pltpu.VMEM((CHIPS, ROWS, HD), BF16),
            pltpu.VMEM((CHIPS, ROWS, HD), BF16),
            pltpu.VMEM((2 * ROWS, HD), F32),
            pltpu.VMEM((NZ, 2, KEYS, HD), F32),
            pltpu.VMEM((2, NZ, KEYS, HD), BF16),
            pltpu.VMEM((2, 2, KEYS, HD), BF16),
            pltpu.VMEM((2, KEYS, HD), BF16),
            pltpu.VMEM((2, 4, KEYS, HD), BF16),
            sem((PEERS - 1,)),
            sem((PEERS,)),
            sem((CHIPS,)),
            sem((CHIPS,)),
            sem((2, NZ)),
            sem((2, NZ)),
            sem((PEERS,)),
            sem((PEERS,)),
            sem((CHIPS,)),
            sem((CHIPS,)),
            sem,
            sem,
            sem((CHIPS,)),
            sem((CHIPS,)),
            sem((2, NZ)),
            sem((2, 2)),
            sem((2,)),
            sem((2, 4)),
        ],
        compiler_params=pltpu.CompilerParams(
            collective_id=0, has_side_effects=True, vmem_limit_bytes=56 * 1024 * 1024
        ),
        name="attention_grads",
    )(queries, grad_out, prefix_keys, prefix_values, cand_keys, cand_values, lengths, offsets)


def solution(mesh):
    torus = Mesh(mesh.devices.reshape(NZ, 2, 2, NY, 2), AXES)
    in_specs = (
        P(CAND_CTX, None),
        P(CAND_CTX, None),
        P(CTX_CAND, None),
        P(CTX_CAND, None),
        P(CAND, None),
        P(CAND, None),
        P(CAND, None),
        P(CAND),
    )
    out_specs = (P(CAND_CTX, None), P(CTX_CAND, None), P(CTX_CAND, None))
    return jax.shard_map(body, mesh=torus, in_specs=in_specs, out_specs=out_specs, check_vma=False)
```

```python
import math

import jax
import jax.numpy as jnp
from jax import lax
from jax.experimental import pallas as pl
from jax.experimental.pallas import tpu as pltpu
from jax.sharding import Mesh
from jax.sharding import PartitionSpec as P

HEADS = 8
HD = 128
NX = NY = 4
NZ = 8
CHIPS = NX * NY
PEERS = 2 * CHIPS
TOK = 8
ROWS = TOK * HEADS
TILE = 4 * ROWS
TILES = PEERS * ROWS // TILE
KEYS = 128
GROUPS = ((0, 2), (2, 5), (5, 8))
SAMPLES = 4
AXES = ("z", "xh", "core", "y", "xl")
CAND = ("y", "xl")
CAND_CTX = ("y", "xl", "z", "xh", "core")
CTX_CAND = ("z", "xh", "core", "y", "xl")
MESH = pl.DeviceIdType.MESH
NEG = -1e30
SCALING = 1.0 / math.sqrt(HD)
SCORE = SCALING * math.log2(math.e)
PLACE = {0: 0, 1: 1, 7: 2, 2: 3, 6: 4, 3: 5, 5: 6, 4: 7}
BACK = {place: r for r, place in PLACE.items()}
STEPS = (0, 1, 3, 2)
BACKWARD = (0, 2, 1, 3)
HOPS = (0, 1, 1, 2)
FAR = [HOPS[r // 4] + HOPS[r % 4] for r in range(CHIPS)]
SEEN = [4 * BACKWARD[r // 4] + BACKWARD[r % 4] for r in range(CHIPS)]
NEAREST = sorted(range(1, CHIPS), key=lambda r: FAR[r])
FARTHEST = NEAREST[::-1]
PIECE = 2 * ROWS + 16
F32 = jnp.float32
BF16 = jnp.bfloat16
NT = (((1,), (1,)), ((), ()))


def stacked(block):
    wide = block.astype(F32)
    return jnp.concatenate([wide[:, h * HD : (h + 1) * HD] for h in range(HEADS)], axis=0)


def kernel(
    q_ref, g_ref, pk_ref, pv_ref, ck_ref, cv_ref, len_ref, off_ref,
    gq_ref, gk_ref, gv_ref,
    qg, kv, kt, e_buf, p_buf, mg, tot, car, loc, ab, stat_out, stat_in, fin_out, fin,
    self_e, self_p, dq_out, dq_mate, dq_sum, dq_in, dq_self, part, rs_out, rs_near, rs_far, rs_end,
    qg_send, qg_recv, kv_send, kv_recv,
    st_send, st_recv, fin_send, fin_recv, mate_send, mate_recv, dq_send, dq_recv,
    rs_send, near_recv, far_recv, end_recv,
):
    z, xh, core, y, xl = (lax.axis_index(a) for a in AXES)
    x = 2 * xh + xl
    other = 1 - core
    mate = {"core": other}
    up, up2, down2, down = ({"z": lax.rem(z + d, NZ)} for d in (1, 2, NZ - 2, NZ - 1))
    chips = []
    for r in range(CHIPS):
        px, py = lax.rem(x + STEPS[r // 4], NX), lax.rem(y + STEPS[r % 4], NY)
        chips.append({"xh": lax.div(px, 2), "xl": lax.rem(px, 2), "y": py})

    first_unit, second_unit = 1 + 3 * core, 4 - 3 * core

    def along(axis, k):
        px = lax.rem(x + STEPS[k] * (core if axis == 0 else other), NX)
        py = lax.rem(y + STEPS[k] * (other if axis == 0 else core), NY)
        return {"xh": lax.div(px, 2), "xl": lax.rem(px, 2), "y": py}

    lines = [[along(axis, k) for k in range(4)] for axis in range(2)]
    sent = []

    def remote(src, dst, send_sem, recv_sem, device):
        return pltpu.make_async_remote_copy(
            src_ref=src, dst_ref=dst, send_sem=send_sem, recv_sem=recv_sem,
            device_id=device, device_id_type=MESH,
        )

    def send(*args):
        copy = remote(*args)
        copy.start()
        sent.append(copy)

    def arrived(dst, send_sem, recv_sem):
        remote(dst, dst, send_sem, recv_sem, mate).wait_recv()

    qg[core, 0:ROWS] = stacked(q_ref[...]).astype(BF16)
    qg[core, ROWS : 2 * ROWS] = stacked(g_ref[...]).astype(BF16)
    kv[0, 0] = pk_ref[...]
    kv[1, 0] = pv_ref[...]

    ends = [len_ref[0, 0]]
    for s in range(1, SAMPLES):
        ends.append(ends[-1] + len_ref[0, s])

    def sample_of(token):
        return sum((token >= end).astype(jnp.int32) for end in ends)

    lane = lax.broadcasted_iota(jnp.int32, (1, 2 * ROWS), 1)
    token = ((z * 2 + xh) * 2 + lax.div(lane, ROWS)) * TOK + lax.rem(lane, TOK)
    sample = sample_of(token)
    high, low = jnp.zeros((1, 2 * ROWS), F32), jnp.zeros((1, 2 * ROWS), F32)
    for s in range(SAMPLES):
        mine = sample == s
        high = jnp.where(mine, lax.div(off_ref[s], 256).astype(F32), high)
        low = jnp.where(mine, lax.rem(off_ref[s], 256).astype(F32), low)
    high, low = (jnp.broadcast_to(part_of, (8, 2 * ROWS)) for part_of in (high, low))
    qg[core, 2 * ROWS : PIECE] = jnp.concatenate([high, low], axis=0).astype(BF16)

    barrier = pltpu.get_barrier_semaphore()
    greeted = [mate, up, down, up2, down2] + lines[0][1:] + lines[1][1:]
    for device in greeted:
        pl.semaphore_signal(barrier, inc=1, device_id=device, device_id_type=MESH)
    pl.semaphore_wait(barrier, len(greeted))

    def kv_to(kind, back, new_back, device):
        src = (pk_ref, pv_ref)[kind] if back == 0 else kv.at[kind, PLACE[back]]
        at = PLACE[new_back]
        send(src, kv.at[kind, at], kv_send.at[kind, at], kv_recv.at[kind, at], device)

    def kv_wait(kind, back):
        at = PLACE[back]
        arrived(kv.at[kind, at], kv_send.at[kind, at], kv_recv.at[kind, at])

    def rows_wait(slot):
        arrived(qg.at[slot], qg_send.at[0], qg_recv.at[slot])

    def slot_of(first, second):
        return 2 * (first * first_unit + second * second_unit) + core

    rows_sent = iter(range(PEERS))

    def rows_to(slot, there, device):
        send(qg.at[slot], qg.at[there], qg_send.at[next(rows_sent)], qg_recv.at[there], device)

    def second_line(first):
        for k in (3, 1, 2):
            rows_to(slot_of(first, 0), slot_of(first, BACKWARD[k]), lines[1][k])

    def rows_from(first, second):
        slot = slot_of(first, second)
        rows_wait(slot)
        if first and not second:
            second_line(first)
        rows_to(slot, slot, mate)

    for kind in range(2):
        kv_to(kind, 0, 2, up2)
        kv_to(kind, 0, 6, down2)
    for k in (3, 1, 2):
        rows_to(core, slot_of(BACKWARD[k], 0), lines[0][k])
    rows_to(core, core, mate)
    second_line(0)
    for kind in range(2):
        kv_to(kind, 0, 1, up)
        kv_to(kind, 0, 7, down)

    rows_wait(other)
    own_q = qg[0:2, 0:ROWS].reshape(2 * ROWS, HD)
    own_g = qg[0:2, ROWS : 2 * ROWS].reshape(2 * ROWS, HD)
    block = ck_ref.shape[0]
    cand_token = lax.broadcasted_iota(jnp.int32, (block, 2 * ROWS), 0)
    allowed = (sample_of(cand_token) == sample) & (cand_token <= token)
    score = lax.dot_general(ck_ref[...], own_q, NT, preferred_element_type=F32) * SCORE
    score = jnp.where(allowed, score, NEG)
    own_high = jnp.max(score, axis=0, keepdims=True)
    expon = jnp.exp2(score - own_high)
    product = lax.dot_general(cv_ref[...], own_g, NT, preferred_element_type=F32)
    own_total = jnp.sum(expon, axis=0, keepdims=True)
    own_carry = jnp.sum(expon * product, axis=0, keepdims=True)
    self_e[...] = expon
    self_p[...] = product

    def first_key(place):
        behind = lax.rem(z + NZ - BACK[place], NZ)
        return (((behind * 2 + xh) * 2 + core) * 8 + y * 2 + xl) * KEYS

    starts = [first_key(place).astype(F32) for place in range(NZ)]

    def first_pass(t, groups):
        rows_q = qg[pl.ds(4 * t, 4), 0:ROWS].reshape(TILE, HD)
        rows_g = qg[pl.ds(4 * t, 4), ROWS : 2 * ROWS].reshape(TILE, HD)
        coded = [qg[4 * t + 2 * i, 2 * ROWS : PIECE].astype(F32) for i in range(2)]
        rows_limit = jnp.concatenate([c[0:1] * 256.0 + c[8:9] for c in coded], axis=1)
        for g in groups:
            low, high = GROUPS[g]
            count = (high - low) * KEYS
            keys = kv[0, low:high].reshape(count, HD)
            values = kv[1, low:high].reshape(count, HD)
            score = lax.dot_general(keys, rows_q, NT, preferred_element_type=F32) * SCORE
            index = lax.broadcasted_iota(jnp.int32, (KEYS, TILE), 0).astype(F32)
            masked = []
            for i, place in enumerate(range(low, high)):
                seen = index < rows_limit - starts[place]
                masked.append(jnp.where(seen, score[i * KEYS : (i + 1) * KEYS], NEG))
            score = jnp.concatenate(masked, axis=0)
            top = jnp.max(score, axis=0, keepdims=True)
            expon = jnp.exp2(score - top)
            product = lax.dot_general(values, rows_g, NT, preferred_element_type=F32)
            e_buf[t, low * KEYS : high * KEYS] = expon
            p_buf[t, low * KEYS : high * KEYS] = product
            mg[t, g : g + 1] = top
            tot[t, g : g + 1] = jnp.sum(expon, axis=0, keepdims=True)
            car[t, g : g + 1] = jnp.sum(expon * product, axis=0, keepdims=True)

    def run_first_pass(start, stop, groups):
        def step(t, carry):
            first_pass(t, groups)
            return carry

        lax.fori_loop(start, stop, step, 0)

    def close_rows(t, carry):
        highs = mg[t]
        top = jnp.max(highs, axis=0, keepdims=True)
        weight = jnp.exp2(highs - top)
        total = jnp.sum(tot[t] * weight, axis=0, keepdims=True)
        carried = jnp.sum(car[t] * weight, axis=0, keepdims=True)
        loc[t] = jnp.concatenate([top, carried / total], axis=0)
        stats = jnp.concatenate([top, total, carried, top], axis=0)
        stat_out[2 * t] = stats[:, : 2 * ROWS]
        stat_out[2 * t + 1] = stats[:, 2 * ROWS :]
        return carry

    def tile_wait(tiles):
        for t in tiles:
            for r in (2 * t, 2 * t + 1):
                if r:
                    rows_wait(2 * r + other)

    for k in (1, 2, 3):
        rows_from(k, 0)
    kv_wait(0, 2)
    kv_to(0, 2, 4, up2)
    kv_to(0, 2, 3, up)
    kv_wait(0, 6)
    kv_to(0, 6, 5, down)
    kv_wait(1, 6)
    kv_to(1, 6, 4, down2)
    kv_to(1, 6, 5, down)
    kv_wait(1, 2)
    kv_to(1, 2, 3, up)
    for k in (1, 2, 3):
        rows_from(0, k)
    for kind in range(2):
        for back in (1, 7):
            kv_wait(kind, back)
    tile_wait((0, 1))
    run_first_pass(0, 2, (0, 1))
    for second in (1, 2, 3):
        for first in (1, 2, 3):
            rows_from(first, second)
    tile_wait((2, 3, 4, 5))
    run_first_pass(2, 6, (0, 1))
    for kind in range(2):
        for back in (3, 5, 4):
            kv_wait(kind, back)
    run_first_pass(0, 6, (2,))
    tile_wait((6, 7))
    run_first_pass(6, TILES, (0, 1, 2))
    lax.fori_loop(0, TILES, close_rows, 0)

    for r in FARTHEST:
        for i, c in enumerate((core, other)):
            slot = 2 * SEEN[r] + core
            send(
                stat_out.at[r], stat_in.at[slot], st_send.at[2 * r + i], st_recv.at[slot],
                {**chips[r], "core": c},
            )
    send(stat_out.at[0], stat_in.at[core], st_send.at[0], st_recv.at[core], mate)
    stat_in[core] = stat_out[0]

    for place in range(NZ):
        kt[:, place * KEYS : (place + 1) * KEYS] = kv[0, place].astype(F32).T.astype(BF16)

    def query_products(t, carry):
        top, delta = loc[t, 0:1], loc[t, 1:2]
        expons, slopes = [], []
        for g, (low, high) in enumerate(GROUPS):
            weight = jnp.exp2(mg[t, g : g + 1] - top)
            expon = e_buf[t, low * KEYS : high * KEYS] * weight
            expons.append(expon.astype(BF16))
            slopes.append((expon * (p_buf[t, low * KEYS : high * KEYS] - delta)).astype(BF16))
        for i, right in enumerate((slopes, expons)):
            ab[t, i] = jnp.dot(kt[...], jnp.concatenate(right, axis=0), preferred_element_type=F32)
        return carry

    lax.fori_loop(0, TILES, query_products, 0)

    arrived(stat_in.at[other], st_send.at[0], st_recv.at[other])
    for r in NEAREST:
        for c in (core, other):
            arrived(stat_in.at[2 * r + c], st_send.at[0], st_recv.at[2 * r + c])
    top = own_high
    for i in range(PEERS):
        top = jnp.maximum(top, stat_in[i][0:1])
    weight = jnp.exp2(own_high - top)
    total, carried = own_total * weight, own_carry * weight
    for i in range(PEERS):
        stats = stat_in[i]
        weight = jnp.exp2(stats[0:1] - top)
        total += stats[1:2] * weight
        carried += stats[2:3] * weight
    inverse = 1.0 / total
    delta = carried * inverse
    final = jnp.concatenate([top, inverse, delta, top], axis=0)
    fin_out[...] = final
    fin[0] = final
    for r in FARTHEST:
        send(fin_out, fin.at[SEEN[r]], fin_send.at[r], fin_recv.at[SEEN[r]], chips[r])

    self_probs = self_e[...] * (jnp.exp2(own_high - top) * inverse)
    self_slopes = (self_probs * (self_p[...] - delta)).astype(BF16)
    self_keys = ck_ref[...].astype(F32).T.astype(BF16)
    dq_self[...] = (jnp.dot(self_keys, self_slopes, preferred_element_type=F32) * SCALING).T

    for r in NEAREST:
        arrived(fin.at[r], fin_send.at[1], fin_recv.at[r])

    def close_weights(t, carry):
        final = jnp.concatenate([fin[2 * t], fin[2 * t + 1]], axis=1)
        mg[t] = jnp.exp2(mg[t] - final[0:1]) * final[1:2]
        return carry

    lax.fori_loop(0, TILES, close_weights, 0)

    def second_pass(place, carry):
        g = lax.div(place + 1, 3)
        grad_k = jnp.zeros((KEYS, HD), F32)
        grad_v = jnp.zeros((KEYS, HD), F32)
        for t in range(TILES):
            delta = jnp.concatenate([fin[2 * t, 2:3], fin[2 * t + 1, 2:3]], axis=1)
            at = pl.ds(pl.multiple_of(place * KEYS, KEYS), KEYS)
            probs = e_buf[t, at] * mg[t, pl.ds(g, 1)]
            slopes = (probs * (p_buf[t, at] - delta)).astype(BF16)
            rows_q = qg[4 * t : 4 * t + 4, 0:ROWS].reshape(TILE, HD)
            rows_g = qg[4 * t : 4 * t + 4, ROWS : 2 * ROWS].reshape(TILE, HD)
            grad_v += jnp.dot(probs.astype(BF16), rows_g, preferred_element_type=F32)
            grad_k += jnp.dot(slopes, rows_q, preferred_element_type=F32)
        part[place, 0] = grad_k * SCALING
        part[place, 1] = grad_v
        return carry

    def pass_on(kind, back, dst, sem, device, *more):
        at = PLACE[back]
        total = part[at, kind]
        for ref in more:
            total = total + ref[...].astype(F32)
        rs_out[kind, at] = total.astype(BF16)
        send(rs_out.at[kind, at], dst, rs_send.at[kind, at], sem, device)

    lax.fori_loop(0, 3, lambda i, c: second_pass(7 - i, c), 0)
    pass_on(0, 4, rs_far.at[0], far_recv.at[0], down2)
    pass_on(1, 4, rs_far.at[1], far_recv.at[1], up2)
    for kind in range(2):
        pass_on(kind, 3, rs_near.at[kind, 0], near_recv.at[kind, 0], down)
        pass_on(kind, 5, rs_near.at[kind, 1], near_recv.at[kind, 1], up)

    def query_pass(t, carry):
        final = jnp.concatenate([fin[2 * t], fin[2 * t + 1]], axis=1)
        weight = jnp.exp2(loc[t, 0:1] - final[0:1]) * final[1:2] * SCALING
        grads = (ab[t, 0] - ab[t, 1] * (final[2:3] - loc[t, 1:2])) * weight
        rows = grads.T.astype(BF16)
        for i in range(2):
            for c in range(2):
                at = (2 * i + c) * ROWS
                dq_out[c, 2 * t + i] = rows[at : at + ROWS]
        return carry

    lax.fori_loop(0, TILES, query_pass, 0)
    send(dq_out.at[other], dq_mate, mate_send, mate_recv, mate)
    lax.fori_loop(0, 3, lambda i, c: second_pass(4 - i, c), 0)
    arrived(dq_mate, mate_send, mate_recv)

    def add_mate(r, carry):
        dq_sum[r] = (dq_out[core, r].astype(F32) + dq_mate[r].astype(F32)).astype(BF16)
        return carry

    lax.fori_loop(0, CHIPS, add_mate, 0)
    for r in FARTHEST:
        send(dq_sum.at[r], dq_in.at[SEEN[r]], dq_send.at[r], dq_recv.at[SEEN[r]], chips[r])
    lax.fori_loop(0, 2, lambda i, c: second_pass(1 - i, c), 0)
    for kind in range(2):
        pass_on(kind, 7, rs_end.at[kind, 2], end_recv.at[kind, 2], up)
        pass_on(kind, 1, rs_end.at[kind, 0], end_recv.at[kind, 0], down)

    def two_on(kind, way):
        arrived(rs_near.at[kind, way], rs_send.at[kind, 0], near_recv.at[kind, way])
        more = [rs_near.at[kind, way]]
        if kind == way:
            arrived(rs_far.at[way], rs_send.at[kind, 0], far_recv.at[way])
            more.append(rs_far.at[way])
        slot = 1 + 2 * way
        device = (down2, up2)[way]
        pass_on(
            kind, (2, 6)[way], rs_end.at[kind, slot], end_recv.at[kind, slot], device, *more
        )

    for kind, way in ((0, 0), (1, 1), (1, 0), (0, 1)):
        two_on(kind, way)

    grads = dq_self[pl.ds(pl.multiple_of(core * ROWS, ROWS), ROWS)] + dq_sum[0].astype(F32)
    for r in NEAREST:
        arrived(dq_in.at[r], dq_send.at[1], dq_recv.at[r])
        grads += dq_in[r].astype(F32)
    gq_ref[...] = jnp.concatenate(
        [grads[h * TOK : (h + 1) * TOK] for h in range(HEADS)], axis=1
    ).astype(BF16)
    for kind, out in enumerate((gk_ref, gv_ref)):
        total = part[0, kind]
        for way in (0, 2, 1, 3):
            arrived(rs_end.at[kind, way], rs_send.at[kind, 0], end_recv.at[kind, way])
            total = total + rs_end[kind, way].astype(F32)
        out[...] = total.astype(BF16)
    for copy in sent:
        copy.wait_send()


def body(queries, grad_out, prefix_keys, prefix_values, cand_keys, cand_values, lengths, offsets):
    vmem = pl.BlockSpec(memory_space=pltpu.VMEM)
    smem = pl.BlockSpec(memory_space=pltpu.SMEM)
    keys = NZ * KEYS
    block = cand_keys.shape[0]
    sem = pltpu.SemaphoreType.DMA
    return pl.pallas_call(
        kernel,
        out_shape=(
            jax.ShapeDtypeStruct(queries.shape, BF16),
            jax.ShapeDtypeStruct(prefix_keys.shape, BF16),
            jax.ShapeDtypeStruct(prefix_values.shape, BF16),
        ),
        in_specs=[vmem] * 6 + [smem] * 2,
        out_specs=(vmem,) * 3,
        scratch_shapes=[
            pltpu.VMEM((PEERS, PIECE, HD), BF16),
            pltpu.VMEM((2, NZ, KEYS, HD), BF16),
            pltpu.VMEM((HD, keys), BF16),
            pltpu.VMEM((TILES, keys, TILE), F32),
            pltpu.VMEM((TILES, keys, TILE), F32),
            pltpu.VMEM((TILES, len(GROUPS), TILE), F32),
            pltpu.VMEM((TILES, len(GROUPS), TILE), F32),
            pltpu.VMEM((TILES, len(GROUPS), TILE), F32),
            pltpu.VMEM((TILES, 2, TILE), F32),
            pltpu.VMEM((TILES, 2, HD, TILE), F32),
            pltpu.VMEM((CHIPS, 4, 2 * ROWS), F32),
            pltpu.VMEM((PEERS, 4, 2 * ROWS), F32),
            pltpu.VMEM((4, 2 * ROWS), F32),
            pltpu.VMEM((CHIPS, 4, 2 * ROWS), F32),
            pltpu.VMEM((block, 2 * ROWS), F32),
            pltpu.VMEM((block, 2 * ROWS), F32),
            pltpu.VMEM((2, CHIPS, ROWS, HD), BF16),
            pltpu.VMEM((CHIPS, ROWS, HD), BF16),
            pltpu.VMEM((CHIPS, ROWS, HD), BF16),
            pltpu.VMEM((CHIPS, ROWS, HD), BF16),
            pltpu.VMEM((2 * ROWS, HD), F32),
            pltpu.VMEM((NZ, 2, KEYS, HD), F32),
            pltpu.VMEM((2, NZ, KEYS, HD), BF16),
            pltpu.VMEM((2, 2, KEYS, HD), BF16),
            pltpu.VMEM((2, KEYS, HD), BF16),
            pltpu.VMEM((2, 4, KEYS, HD), BF16),
            sem((PEERS,)),
            sem((PEERS,)),
            sem((2, NZ)),
            sem((2, NZ)),
            sem((PEERS,)),
            sem((PEERS,)),
            sem((CHIPS,)),
            sem((CHIPS,)),
            sem,
            sem,
            sem((CHIPS,)),
            sem((CHIPS,)),
            sem((2, NZ)),
            sem((2, 2)),
            sem((2,)),
            sem((2, 4)),
        ],
        compiler_params=pltpu.CompilerParams(
            collective_id=0, has_side_effects=True, vmem_limit_bytes=56 * 1024 * 1024
        ),
        name="attention_grads",
    )(queries, grad_out, prefix_keys, prefix_values, cand_keys, cand_values, lengths, offsets)


def solution(mesh):
    torus = Mesh(mesh.devices.reshape(NZ, 2, 2, NY, 2), AXES)
    in_specs = (
        P(CAND_CTX, None),
        P(CAND_CTX, None),
        P(CTX_CAND, None),
        P(CTX_CAND, None),
        P(CAND, None),
        P(CAND, None),
        P(CAND, None),
        P(CAND),
    )
    out_specs = (P(CAND_CTX, None), P(CTX_CAND, None), P(CTX_CAND, None))
    return jax.shard_map(body, mesh=torus, in_specs=in_specs, out_specs=out_specs, check_vma=False)
```

```python
import math

import jax
import jax.numpy as jnp
from jax import lax
from jax.experimental import pallas as pl
from jax.experimental.pallas import tpu as pltpu
from jax.sharding import Mesh
from jax.sharding import PartitionSpec as P

HEADS = 8
HD = 128
NX = NY = 4
NZ = 8
CHIPS = NX * NY
PEERS = 2 * CHIPS
TOK = 8
ROWS = TOK * HEADS
TILE = 4 * ROWS
TILES = PEERS * ROWS // TILE
KEYS = 128
GROUPS = ((0, 2), (2, 5), (5, 8))
SAMPLES = 4
AXES = ("z", "xh", "core", "y", "xl")
CAND = ("y", "xl")
CAND_CTX = ("y", "xl", "z", "xh", "core")
CTX_CAND = ("z", "xh", "core", "y", "xl")
MESH = pl.DeviceIdType.MESH
NEG = -1e30
SCALING = 1.0 / math.sqrt(HD)
SCORE = SCALING * math.log2(math.e)
PLACE = {0: 0, 1: 1, 7: 2, 2: 3, 6: 4, 3: 5, 5: 6, 4: 7}
BACK = {place: r for r, place in PLACE.items()}
STEPS = (0, 1, 3, 2)
BACKWARD = (0, 2, 1, 3)
HOPS = (0, 1, 1, 2)
ORDER = (
    (0, 0), (0, 1), (1, 0), (0, 2), (2, 0), (0, 3), (3, 0), (1, 1),
    (2, 1), (1, 2), (2, 2), (1, 3), (3, 1), (2, 3), (3, 2), (3, 3),
)
FAR = [HOPS[a] + HOPS[b] for a, b in ORDER]
SEEN = [ORDER.index((BACKWARD[a], BACKWARD[b])) for a, b in ORDER]
NEAREST = sorted(range(1, CHIPS), key=lambda r: FAR[r])
FARTHEST = NEAREST[::-1]
PIECE = 2 * ROWS + 16
F32 = jnp.float32
BF16 = jnp.bfloat16
NT = (((1,), (1,)), ((), ()))


def stacked(block):
    wide = block.astype(F32)
    return jnp.concatenate([wide[:, h * HD : (h + 1) * HD] for h in range(HEADS)], axis=0)


def kernel(
    q_hbm, g_hbm, pk_hbm, pv_hbm, ck_hbm, cv_hbm, len_hbm, off_hbm,
    gq_ref, gk_ref, gv_ref,
    q_ref, g_ref, ck_ref, cv_ref, len_ref, off_ref, in_sem, qg, kv, kt, e_buf, p_buf, mg, tot, car, loc, ab, stat_out, stat_in, fin_out, fin,
    self_e, self_p, dq_out, dq_mate, dq_sum, dq_in, dq_self, part, rs_out, rs_near, rs_far, rs_end,
    qg_send, qg_recv, kv_send, kv_recv,
    st_send, st_recv, fin_send, fin_recv, mate_send, mate_recv, dq_send, dq_recv,
    rs_send, near_recv, far_recv, end_recv,
):
    z, xh, core, y, xl = (lax.axis_index(a) for a in AXES)
    x = 2 * xh + xl
    other = 1 - core
    mate = {"core": other}
    up, up2, down2, down = ({"z": lax.rem(z + d, NZ)} for d in (1, 2, NZ - 2, NZ - 1))
    chips = []
    for r in range(CHIPS):
        px, py = lax.rem(x + STEPS[ORDER[r][0]], NX), lax.rem(y + STEPS[ORDER[r][1]], NY)
        chips.append({"xh": lax.div(px, 2), "xl": lax.rem(px, 2), "y": py})

    def along(axis, k):
        px = lax.rem(x + STEPS[k] * (core if axis == 0 else other), NX)
        py = lax.rem(y + STEPS[k] * (other if axis == 0 else core), NY)
        return {"xh": lax.div(px, 2), "xl": lax.rem(px, 2), "y": py}

    lines = [[along(axis, k) for k in range(4)] for axis in range(2)]
    sent = []

    def remote(src, dst, send_sem, recv_sem, device):
        return pltpu.make_async_remote_copy(
            src_ref=src, dst_ref=dst, send_sem=send_sem, recv_sem=recv_sem,
            device_id=device, device_id_type=MESH,
        )

    def send(*args):
        copy = remote(*args)
        copy.start()
        sent.append(copy)

    def arrived(dst, send_sem, recv_sem):
        remote(dst, dst, send_sem, recv_sem, mate).wait_recv()

    inputs = [
        pltpu.make_async_copy(src, dst, in_sem.at[i])
        for i, (src, dst) in enumerate(
            (
                (pk_hbm, kv.at[0, 0]), (pv_hbm, kv.at[1, 0]), (q_hbm, q_ref), (g_hbm, g_ref),
                (len_hbm, len_ref), (off_hbm, off_ref), (ck_hbm, ck_ref), (cv_hbm, cv_ref),
            )
        )
    ]
    for copy in inputs:
        copy.start()
    barrier = pltpu.get_barrier_semaphore()
    greeted = [mate, up, down, up2, down2] + lines[0][1:] + lines[1][1:]
    for device in greeted:
        pl.semaphore_signal(barrier, inc=1, device_id=device, device_id_type=MESH)
    for copy in inputs[2:6]:
        copy.wait()

    qg[core, 0:ROWS] = stacked(q_ref[...]).astype(BF16)
    qg[core, ROWS : 2 * ROWS] = stacked(g_ref[...]).astype(BF16)

    ends = [len_ref[0, 0]]
    for s in range(1, SAMPLES):
        ends.append(ends[-1] + len_ref[0, s])

    def sample_of(token):
        return sum((token >= end).astype(jnp.int32) for end in ends)

    lane = lax.broadcasted_iota(jnp.int32, (1, 2 * ROWS), 1)
    token = ((z * 2 + xh) * 2 + lax.div(lane, ROWS)) * TOK + lax.rem(lane, TOK)
    sample = sample_of(token)
    high, low = jnp.zeros((1, 2 * ROWS), F32), jnp.zeros((1, 2 * ROWS), F32)
    for s in range(SAMPLES):
        mine = sample == s
        high = jnp.where(mine, lax.div(off_ref[s], 256).astype(F32), high)
        low = jnp.where(mine, lax.rem(off_ref[s], 256).astype(F32), low)
    high, low = (jnp.broadcast_to(part_of, (8, 2 * ROWS)) for part_of in (high, low))
    qg[core, 2 * ROWS : PIECE] = jnp.concatenate([high, low], axis=0).astype(BF16)

    for copy in inputs[:2]:
        copy.wait()
    pl.semaphore_wait(barrier, len(greeted))

    def kv_to(kind, back, new_back, device):
        at = PLACE[new_back]
        send(kv.at[kind, PLACE[back]], kv.at[kind, at], kv_send.at[kind, at], kv_recv.at[kind, at], device)

    def kv_wait(kind, back):
        at = PLACE[back]
        arrived(kv.at[kind, at], kv_send.at[kind, at], kv_recv.at[kind, at])

    def rows_wait(slot):
        arrived(qg.at[slot], qg_send.at[0], qg_recv.at[slot])

    def slot_of(first, second):
        return 2 * (other * ORDER.index((second, first)) + core * ORDER.index((first, second))) + core

    rows_sent = iter(range(PEERS))

    def rows_to(slot, there, device):
        send(qg.at[slot], qg.at[there], qg_send.at[next(rows_sent)], qg_recv.at[there], device)

    def second_line(first):
        for k in (3, 1, 2):
            rows_to(slot_of(first, 0), slot_of(first, BACKWARD[k]), lines[1][k])

    def rows_from(first, second):
        slot = slot_of(first, second)
        rows_wait(slot)
        if first and not second:
            second_line(first)
        rows_to(slot, slot, mate)

    for kind in range(2):
        kv_to(kind, 0, 2, up2)
        kv_to(kind, 0, 6, down2)
    for k in (3, 1, 2):
        rows_to(core, slot_of(BACKWARD[k], 0), lines[0][k])
    rows_to(core, core, mate)
    second_line(0)
    for kind in range(2):
        kv_to(kind, 0, 1, up)
        kv_to(kind, 0, 7, down)

    for copy in inputs[6:]:
        copy.wait()
    rows_wait(other)
    own_q = qg[0:2, 0:ROWS].reshape(2 * ROWS, HD)
    own_g = qg[0:2, ROWS : 2 * ROWS].reshape(2 * ROWS, HD)
    block = ck_ref.shape[0]
    cand_token = lax.broadcasted_iota(jnp.int32, (block, 2 * ROWS), 0)
    allowed = (sample_of(cand_token) == sample) & (cand_token <= token)
    score = lax.dot_general(ck_ref[...], own_q, NT, preferred_element_type=F32) * SCORE
    score = jnp.where(allowed, score, NEG)
    own_high = jnp.max(score, axis=0, keepdims=True)
    expon = jnp.exp2(score - own_high)
    product = lax.dot_general(cv_ref[...], own_g, NT, preferred_element_type=F32)
    own_total = jnp.sum(expon, axis=0, keepdims=True)
    own_carry = jnp.sum(expon * product, axis=0, keepdims=True)
    self_e[...] = expon
    self_p[...] = product

    def first_key(place):
        behind = lax.rem(z + NZ - BACK[place], NZ)
        return (((behind * 2 + xh) * 2 + core) * 8 + y * 2 + xl) * KEYS

    starts = [first_key(place).astype(F32) for place in range(NZ)]

    def first_pass(t, groups):
        rows_q = qg[pl.ds(4 * t, 4), 0:ROWS].reshape(TILE, HD)
        rows_g = qg[pl.ds(4 * t, 4), ROWS : 2 * ROWS].reshape(TILE, HD)
        coded = [qg[4 * t + 2 * i, 2 * ROWS : PIECE].astype(F32) for i in range(2)]
        rows_limit = jnp.concatenate([c[0:1] * 256.0 + c[8:9] for c in coded], axis=1)
        for g in groups:
            low, high = GROUPS[g]
            count = (high - low) * KEYS
            keys = kv[0, low:high].reshape(count, HD)
            values = kv[1, low:high].reshape(count, HD)
            score = lax.dot_general(keys, rows_q, NT, preferred_element_type=F32) * SCORE
            index = lax.broadcasted_iota(jnp.int32, (KEYS, TILE), 0).astype(F32)
            masked = []
            for i, place in enumerate(range(low, high)):
                seen = index < rows_limit - starts[place]
                masked.append(jnp.where(seen, score[i * KEYS : (i + 1) * KEYS], NEG))
            score = jnp.concatenate(masked, axis=0)
            top = jnp.max(score, axis=0, keepdims=True)
            expon = jnp.exp2(score - top)
            product = lax.dot_general(values, rows_g, NT, preferred_element_type=F32)
            e_buf[t, low * KEYS : high * KEYS] = expon
            p_buf[t, low * KEYS : high * KEYS] = product
            mg[t, g : g + 1] = top
            tot[t, g : g + 1] = jnp.sum(expon, axis=0, keepdims=True)
            car[t, g : g + 1] = jnp.sum(expon * product, axis=0, keepdims=True)

    def run_first_pass(start, stop, groups):
        def step(t, carry):
            first_pass(t, groups)
            return carry

        lax.fori_loop(start, stop, step, 0)

    def close_rows(t, carry):
        highs = mg[t]
        top = jnp.max(highs, axis=0, keepdims=True)
        weight = jnp.exp2(highs - top)
        total = jnp.sum(tot[t] * weight, axis=0, keepdims=True)
        carried = jnp.sum(car[t] * weight, axis=0, keepdims=True)
        loc[t] = jnp.concatenate([top, carried / total], axis=0)
        stats = jnp.concatenate([top, total, carried, top], axis=0)
        stat_out[2 * t] = stats[:, : 2 * ROWS]
        stat_out[2 * t + 1] = stats[:, 2 * ROWS :]
        return carry

    def tile_wait(tiles):
        for t in tiles:
            for r in (2 * t, 2 * t + 1):
                if not (isinstance(r, int) and r == 0):
                    rows_wait(2 * r + other)

    for k in (1, 2, 3):
        rows_from(k, 0)
    kv_wait(0, 2)
    kv_to(0, 2, 4, up2)
    kv_to(0, 2, 3, up)
    kv_wait(0, 6)
    kv_to(0, 6, 5, down)
    kv_wait(1, 6)
    kv_to(1, 6, 4, down2)
    kv_to(1, 6, 5, down)
    kv_wait(1, 2)
    kv_to(1, 2, 3, up)
    for k in (1, 2, 3):
        rows_from(0, k)
    for kind in range(2):
        for back in (1, 7):
            kv_wait(kind, back)
    tile_wait((0, 1, 2))
    run_first_pass(0, 3, (0, 1))
    for first, second in ((1, 1), (2, 1), (1, 2), (2, 2)):
        rows_from(first, second)
    for kind in range(2):
        for back in (3, 5, 4):
            kv_wait(kind, back)
    run_first_pass(0, 3, (2,))
    for first, second in ((3, 1), (3, 2), (1, 3), (2, 3), (3, 3)):
        rows_from(first, second)

    def last_tiles(t, carry):
        tile_wait((t,))
        first_pass(t, (0, 1, 2))
        return carry

    lax.fori_loop(3, TILES, last_tiles, 0)
    lax.fori_loop(0, TILES, close_rows, 0)

    for r in FARTHEST:
        for i, c in enumerate((core, other)):
            slot = 2 * SEEN[r] + core
            send(
                stat_out.at[r], stat_in.at[slot], st_send.at[2 * r + i], st_recv.at[slot],
                {**chips[r], "core": c},
            )
    send(stat_out.at[0], stat_in.at[core], st_send.at[0], st_recv.at[core], mate)
    stat_in[core] = stat_out[0]

    for place in range(NZ):
        kt[:, place * KEYS : (place + 1) * KEYS] = kv[0, place].astype(F32).T.astype(BF16)

    def query_products(t, carry):
        top, delta = loc[t, 0:1], loc[t, 1:2]
        expons, slopes = [], []
        for g, (low, high) in enumerate(GROUPS):
            weight = jnp.exp2(mg[t, g : g + 1] - top)
            expon = e_buf[t, low * KEYS : high * KEYS] * weight
            expons.append(expon.astype(BF16))
            slopes.append((expon * (p_buf[t, low * KEYS : high * KEYS] - delta)).astype(BF16))
        for i, right in enumerate((slopes, expons)):
            ab[t, i] = jnp.dot(kt[...], jnp.concatenate(right, axis=0), preferred_element_type=F32)
        return carry

    lax.fori_loop(0, TILES, query_products, 0)

    arrived(stat_in.at[other], st_send.at[0], st_recv.at[other])
    for r in NEAREST:
        for c in (core, other):
            arrived(stat_in.at[2 * r + c], st_send.at[0], st_recv.at[2 * r + c])
    top = own_high
    for i in range(PEERS):
        top = jnp.maximum(top, stat_in[i][0:1])
    weight = jnp.exp2(own_high - top)
    total, carried = own_total * weight, own_carry * weight
    for i in range(PEERS):
        stats = stat_in[i]
        weight = jnp.exp2(stats[0:1] - top)
        total += stats[1:2] * weight
        carried += stats[2:3] * weight
    inverse = 1.0 / total
    delta = carried * inverse
    final = jnp.concatenate([top, inverse, delta, top], axis=0)
    fin_out[...] = final
    fin[0] = final
    for r in FARTHEST:
        send(fin_out, fin.at[SEEN[r]], fin_send.at[r], fin_recv.at[SEEN[r]], chips[r])

    self_probs = self_e[...] * (jnp.exp2(own_high - top) * inverse)
    self_slopes = (self_probs * (self_p[...] - delta)).astype(BF16)
    self_keys = ck_ref[...].astype(F32).T.astype(BF16)
    dq_self[...] = (jnp.dot(self_keys, self_slopes, preferred_element_type=F32) * SCALING).T

    for r in NEAREST:
        arrived(fin.at[r], fin_send.at[1], fin_recv.at[r])

    def close_weights(t, carry):
        final = jnp.concatenate([fin[2 * t], fin[2 * t + 1]], axis=1)
        mg[t] = jnp.exp2(mg[t] - final[0:1]) * final[1:2]
        return carry

    lax.fori_loop(0, TILES, close_weights, 0)

    def second_pass(place, carry):
        g = lax.div(place + 1, 3)
        grad_k = jnp.zeros((KEYS, HD), F32)
        grad_v = jnp.zeros((KEYS, HD), F32)
        for t in range(TILES):
            delta = jnp.concatenate([fin[2 * t, 2:3], fin[2 * t + 1, 2:3]], axis=1)
            at = pl.ds(pl.multiple_of(place * KEYS, KEYS), KEYS)
            probs = e_buf[t, at] * mg[t, pl.ds(g, 1)]
            slopes = (probs * (p_buf[t, at] - delta)).astype(BF16)
            rows_q = qg[4 * t : 4 * t + 4, 0:ROWS].reshape(TILE, HD)
            rows_g = qg[4 * t : 4 * t + 4, ROWS : 2 * ROWS].reshape(TILE, HD)
            grad_v += jnp.dot(probs.astype(BF16), rows_g, preferred_element_type=F32)
            grad_k += jnp.dot(slopes, rows_q, preferred_element_type=F32)
        part[place, 0] = grad_k * SCALING
        part[place, 1] = grad_v
        return carry

    def pass_on(kind, back, dst, sem, device, *more):
        at = PLACE[back]
        total = part[at, kind]
        for ref in more:
            total = total + ref[...].astype(F32)
        rs_out[kind, at] = total.astype(BF16)
        send(rs_out.at[kind, at], dst, rs_send.at[kind, at], sem, device)

    second_pass(PLACE[4], 0)
    pass_on(0, 4, rs_far.at[0], far_recv.at[0], down2)
    pass_on(1, 4, rs_far.at[1], far_recv.at[1], up2)
    second_pass(PLACE[3], 0)
    for kind in range(2):
        pass_on(kind, 3, rs_near.at[kind, 0], near_recv.at[kind, 0], down)
    second_pass(PLACE[5], 0)
    for kind in range(2):
        pass_on(kind, 5, rs_near.at[kind, 1], near_recv.at[kind, 1], up)

    def query_pass(t, carry):
        final = jnp.concatenate([fin[2 * t], fin[2 * t + 1]], axis=1)
        weight = jnp.exp2(loc[t, 0:1] - final[0:1]) * final[1:2] * SCALING
        grads = (ab[t, 0] - ab[t, 1] * (final[2:3] - loc[t, 1:2])) * weight
        rows = grads.T.astype(BF16)
        for i in range(2):
            for c in range(2):
                at = (2 * i + c) * ROWS
                dq_out[c, 2 * t + i] = rows[at : at + ROWS]
        return carry

    lax.fori_loop(0, TILES, query_pass, 0)
    send(dq_out.at[other], dq_mate, mate_send, mate_recv, mate)
    lax.fori_loop(0, 2, lambda i, c: second_pass(2 - i, c), 0)
    for kind in range(2):
        pass_on(kind, 7, rs_end.at[kind, 2], end_recv.at[kind, 2], up)
        pass_on(kind, 1, rs_end.at[kind, 0], end_recv.at[kind, 0], down)
    arrived(dq_mate, mate_send, mate_recv)

    def add_mate(r, carry):
        dq_sum[r] = (dq_out[core, r].astype(F32) + dq_mate[r].astype(F32)).astype(BF16)
        return carry

    lax.fori_loop(0, CHIPS, add_mate, 0)
    for r in FARTHEST:
        send(dq_sum.at[r], dq_in.at[SEEN[r]], dq_send.at[r], dq_recv.at[SEEN[r]], chips[r])
    lax.fori_loop(0, 2, lambda i, c: second_pass(4 - i, c), 0)

    def two_on(kind, way):
        arrived(rs_near.at[kind, way], rs_send.at[kind, 0], near_recv.at[kind, way])
        more = [rs_near.at[kind, way]]
        if kind == way:
            arrived(rs_far.at[way], rs_send.at[kind, 0], far_recv.at[way])
            more.append(rs_far.at[way])
        slot = 1 + 2 * way
        device = (down2, up2)[way]
        pass_on(
            kind, (2, 6)[way], rs_end.at[kind, slot], end_recv.at[kind, slot], device, *more
        )

    for kind, way in ((1, 0), (0, 1), (0, 0), (1, 1)):
        two_on(kind, way)
    second_pass(0, 0)

    grads = dq_self[pl.ds(pl.multiple_of(core * ROWS, ROWS), ROWS)] + dq_sum[0].astype(F32)
    for r in NEAREST:
        arrived(dq_in.at[r], dq_send.at[1], dq_recv.at[r])
        grads += dq_in[r].astype(F32)
    gq_ref[...] = jnp.concatenate(
        [grads[h * TOK : (h + 1) * TOK] for h in range(HEADS)], axis=1
    ).astype(BF16)
    for kind, out in enumerate((gk_ref, gv_ref)):
        total = part[0, kind]
        for way in (0, 2, 1, 3):
            arrived(rs_end.at[kind, way], rs_send.at[kind, 0], end_recv.at[kind, way])
            total = total + rs_end[kind, way].astype(F32)
        out[...] = total.astype(BF16)
    for copy in sent:
        copy.wait_send()


def store(*refs):
    sems = refs[6]
    copies = [pltpu.make_async_copy(refs[i], refs[3 + i], sems.at[i]) for i in range(3)]
    for copy in copies:
        copy.start()
    for copy in copies:
        copy.wait()


def body(queries, grad_out, prefix_keys, prefix_values, cand_keys, cand_values, lengths, offsets):
    vmem = pl.BlockSpec(memory_space=pltpu.VMEM)
    anywhere = pl.BlockSpec(memory_space=pl.ANY)
    keys = NZ * KEYS
    block = cand_keys.shape[0]
    sem = pltpu.SemaphoreType.DMA
    found = pl.pallas_call(
        kernel,
        out_shape=(
            pltpu.VMEM(queries.shape, BF16),
            pltpu.VMEM(prefix_keys.shape, BF16),
            pltpu.VMEM(prefix_values.shape, BF16),
        ),
        in_specs=[anywhere] * 8,
        out_specs=(vmem,) * 3,
        scratch_shapes=[
            pltpu.VMEM(queries.shape, BF16),
            pltpu.VMEM(grad_out.shape, BF16),
            pltpu.VMEM(cand_keys.shape, BF16),
            pltpu.VMEM(cand_values.shape, BF16),
            pltpu.SMEM(lengths.shape, jnp.int32),
            pltpu.SMEM(offsets.shape, jnp.int32),
            sem((8,)),
            pltpu.VMEM((PEERS, PIECE, HD), BF16),
            pltpu.VMEM((2, NZ, KEYS, HD), BF16),
            pltpu.VMEM((HD, keys), BF16),
            pltpu.VMEM((TILES, keys, TILE), F32),
            pltpu.VMEM((TILES, keys, TILE), F32),
            pltpu.VMEM((TILES, len(GROUPS), TILE), F32),
            pltpu.VMEM((TILES, len(GROUPS), TILE), F32),
            pltpu.VMEM((TILES, len(GROUPS), TILE), F32),
            pltpu.VMEM((TILES, 2, TILE), F32),
            pltpu.VMEM((TILES, 2, HD, TILE), F32),
            pltpu.VMEM((CHIPS, 4, 2 * ROWS), F32),
            pltpu.VMEM((PEERS, 4, 2 * ROWS), F32),
            pltpu.VMEM((4, 2 * ROWS), F32),
            pltpu.VMEM((CHIPS, 4, 2 * ROWS), F32),
            pltpu.VMEM((block, 2 * ROWS), F32),
            pltpu.VMEM((block, 2 * ROWS), F32),
            pltpu.VMEM((2, CHIPS, ROWS, HD), BF16),
            pltpu.VMEM((CHIPS, ROWS, HD), BF16),
            pltpu.VMEM((CHIPS, ROWS, HD), BF16),
            pltpu.VMEM((CHIPS, ROWS, HD), BF16),
            pltpu.VMEM((2 * ROWS, HD), F32),
            pltpu.VMEM((NZ, 2, KEYS, HD), F32),
            pltpu.VMEM((2, NZ, KEYS, HD), BF16),
            pltpu.VMEM((2, 2, KEYS, HD), BF16),
            pltpu.VMEM((2, KEYS, HD), BF16),
            pltpu.VMEM((2, 4, KEYS, HD), BF16),
            sem((PEERS,)),
            sem((PEERS,)),
            sem((2, NZ)),
            sem((2, NZ)),
            sem((PEERS,)),
            sem((PEERS,)),
            sem((CHIPS,)),
            sem((CHIPS,)),
            sem,
            sem,
            sem((CHIPS,)),
            sem((CHIPS,)),
            sem((2, NZ)),
            sem((2, 2)),
            sem((2,)),
            sem((2, 4)),
        ],
        compiler_params=pltpu.CompilerParams(
            collective_id=0, has_side_effects=True, vmem_limit_bytes=56 * 1024 * 1024
        ),
        name="attention_grads",
    )(queries, grad_out, prefix_keys, prefix_values, cand_keys, cand_values, lengths, offsets)
    return pl.pallas_call(
        store,
        out_shape=tuple(jax.ShapeDtypeStruct(a.shape, BF16) for a in found),
        in_specs=[vmem] * 3,
        out_specs=(anywhere,) * 3,
        scratch_shapes=[sem((3,))],
        name="store",
    )(*(pltpu.with_memory_space_constraint(a, pltpu.VMEM) for a in found))


def solution(mesh):
    torus = Mesh(mesh.devices.reshape(NZ, 2, 2, NY, 2), AXES)
    in_specs = (
        P(CAND_CTX, None),
        P(CAND_CTX, None),
        P(CTX_CAND, None),
        P(CTX_CAND, None),
        P(CAND, None),
        P(CAND, None),
        P(CAND, None),
        P(CAND),
    )
    out_specs = (P(CAND_CTX, None), P(CTX_CAND, None), P(CTX_CAND, None))
    return jax.shard_map(body, mesh=torus, in_specs=in_specs, out_specs=out_specs, check_vma=False)
```

```python
import math

import jax
import jax.numpy as jnp
from jax import lax
from jax.experimental import pallas as pl
from jax.experimental.pallas import tpu as pltpu
from jax.sharding import Mesh
from jax.sharding import PartitionSpec as P

HEADS = 8
HD = 128
NX = NY = 4
NZ = 8
CHIPS = NX * NY
PEERS = 2 * CHIPS
TOK = 8
ROWS = TOK * HEADS
TILE = 4 * ROWS
TILES = PEERS * ROWS // TILE
KEYS = 128
GROUPS = ((0, 2), (2, 5), (5, 8))
SAMPLES = 4
AXES = ("z", "xh", "core", "y", "xl")
CAND = ("y", "xl")
CAND_CTX = ("y", "xl", "z", "xh", "core")
CTX_CAND = ("z", "xh", "core", "y", "xl")
MESH = pl.DeviceIdType.MESH
NEG = -1e30
SCALING = 1.0 / math.sqrt(HD)
SCORE = SCALING * math.log2(math.e)
PLACE = {0: 0, 1: 1, 7: 2, 2: 3, 6: 4, 3: 5, 5: 6, 4: 7}
BACK = {place: r for r, place in PLACE.items()}
STEPS = (0, 1, 3, 2)
BACKWARD = (0, 2, 1, 3)
HOPS = (0, 1, 1, 2)
ORDER = (
    (0, 0), (0, 1), (1, 0), (0, 2), (2, 0), (0, 3), (3, 0), (1, 1),
    (2, 1), (1, 2), (2, 2), (1, 3), (3, 1), (2, 3), (3, 2), (3, 3),
)
FAR = [HOPS[a] + HOPS[b] for a, b in ORDER]
SEEN = [ORDER.index((BACKWARD[a], BACKWARD[b])) for a, b in ORDER]
NEAREST = sorted(range(1, CHIPS), key=lambda r: FAR[r])
FARTHEST = NEAREST[::-1]
PIECE = 2 * ROWS + 16
F32 = jnp.float32
BF16 = jnp.bfloat16
NT = (((1,), (1,)), ((), ()))


def stacked(block):
    wide = block.astype(F32)
    return jnp.concatenate([wide[:, h * HD : (h + 1) * HD] for h in range(HEADS)], axis=0)


def kernel(
    q_hbm, g_hbm, pk_hbm, pv_hbm, ck_hbm, cv_hbm, len_hbm, off_hbm,
    gq_ref, gk_ref, gv_ref,
    q_ref, g_ref, ck_ref, cv_ref, len_ref, off_ref, in_sem, qg, kv, kt, e_buf, p_buf, mg, tot, car, loc, ab, ab_mate, stat_out, stat_in, stat_mate, fin_out, fin,
    self_e, self_p, dq_out, dq_in, dq_self, part, rs_out, rs_near, rs_far, rs_end,
    qg_send, qg_recv, kv_send, kv_recv,
    st_send, st_recv, fin_send, fin_recv, mate_send, mate_recv, ab_send, ab_recv, dq_send, dq_recv,
    rs_send, near_recv, far_recv, end_recv,
):
    z, xh, core, y, xl = (lax.axis_index(a) for a in AXES)
    x = 2 * xh + xl
    other = 1 - core
    mate = {"core": other}
    up, up2, down2, down = ({"z": lax.rem(z + d, NZ)} for d in (1, 2, NZ - 2, NZ - 1))
    chips = []
    for r in range(CHIPS):
        px, py = lax.rem(x + STEPS[ORDER[r][0]], NX), lax.rem(y + STEPS[ORDER[r][1]], NY)
        chips.append({"xh": lax.div(px, 2), "xl": lax.rem(px, 2), "y": py})

    def along(axis, k):
        px = lax.rem(x + STEPS[k] * (core if axis == 0 else other), NX)
        py = lax.rem(y + STEPS[k] * (other if axis == 0 else core), NY)
        return {"xh": lax.div(px, 2), "xl": lax.rem(px, 2), "y": py}

    lines = [[along(axis, k) for k in range(4)] for axis in range(2)]
    sent = []

    def remote(src, dst, send_sem, recv_sem, device):
        return pltpu.make_async_remote_copy(
            src_ref=src, dst_ref=dst, send_sem=send_sem, recv_sem=recv_sem,
            device_id=device, device_id_type=MESH,
        )

    def send(*args):
        copy = remote(*args)
        copy.start()
        sent.append(copy)

    def arrived(dst, send_sem, recv_sem):
        remote(dst, dst, send_sem, recv_sem, mate).wait_recv()

    inputs = [
        pltpu.make_async_copy(src, dst, in_sem.at[i])
        for i, (src, dst) in enumerate(
            (
                (pk_hbm, kv.at[0, 0]), (pv_hbm, kv.at[1, 0]), (q_hbm, q_ref), (g_hbm, g_ref),
                (len_hbm, len_ref), (off_hbm, off_ref), (ck_hbm, ck_ref), (cv_hbm, cv_ref),
            )
        )
    ]
    for copy in inputs:
        copy.start()
    barrier = pltpu.get_barrier_semaphore()
    greeted = [mate, up, down, up2, down2] + lines[0][1:] + lines[1][1:]
    for device in greeted:
        pl.semaphore_signal(barrier, inc=1, device_id=device, device_id_type=MESH)
    for copy in inputs[2:6]:
        copy.wait()

    qg[core, 0:ROWS] = stacked(q_ref[...]).astype(BF16)
    qg[core, ROWS : 2 * ROWS] = stacked(g_ref[...]).astype(BF16)

    ends = [len_ref[0, 0]]
    for s in range(1, SAMPLES):
        ends.append(ends[-1] + len_ref[0, s])

    def sample_of(token):
        return sum((token >= end).astype(jnp.int32) for end in ends)

    lane = lax.broadcasted_iota(jnp.int32, (1, 2 * ROWS), 1)
    token = ((z * 2 + xh) * 2 + lax.div(lane, ROWS)) * TOK + lax.rem(lane, TOK)
    sample = sample_of(token)
    high, low = jnp.zeros((1, 2 * ROWS), F32), jnp.zeros((1, 2 * ROWS), F32)
    for s in range(SAMPLES):
        mine = sample == s
        high = jnp.where(mine, lax.div(off_ref[s], 256).astype(F32), high)
        low = jnp.where(mine, lax.rem(off_ref[s], 256).astype(F32), low)
    high, low = (jnp.broadcast_to(part_of, (8, 2 * ROWS)) for part_of in (high, low))
    qg[core, 2 * ROWS : PIECE] = jnp.concatenate([high, low], axis=0).astype(BF16)

    for copy in inputs[:2]:
        copy.wait()
    pl.semaphore_wait(barrier, len(greeted))

    def kv_to(kind, back, new_back, device):
        at = PLACE[new_back]
        send(kv.at[kind, PLACE[back]], kv.at[kind, at], kv_send.at[kind, at], kv_recv.at[kind, at], device)

    def kv_wait(kind, back):
        at = PLACE[back]
        arrived(kv.at[kind, at], kv_send.at[kind, at], kv_recv.at[kind, at])

    def rows_wait(slot):
        arrived(qg.at[slot], qg_send.at[0], qg_recv.at[slot])

    def slot_of(first, second):
        return 2 * (other * ORDER.index((second, first)) + core * ORDER.index((first, second))) + core

    rows_sent = iter(range(PEERS))

    def rows_to(slot, there, device):
        send(qg.at[slot], qg.at[there], qg_send.at[next(rows_sent)], qg_recv.at[there], device)

    def second_line(first):
        for k in (3, 1, 2):
            rows_to(slot_of(first, 0), slot_of(first, BACKWARD[k]), lines[1][k])

    def rows_from(first, second):
        slot = slot_of(first, second)
        rows_wait(slot)
        if first and not second:
            second_line(first)
        rows_to(slot, slot, mate)

    for kind in range(2):
        kv_to(kind, 0, 2, up2)
        kv_to(kind, 0, 6, down2)
    for k in (3, 1, 2):
        rows_to(core, slot_of(BACKWARD[k], 0), lines[0][k])
    rows_to(core, core, mate)
    second_line(0)
    for kind in range(2):
        kv_to(kind, 0, 1, up)
        kv_to(kind, 0, 7, down)

    for copy in inputs[6:]:
        copy.wait()
    rows_wait(other)
    own_q = qg[0:2, 0:ROWS].reshape(2 * ROWS, HD)
    own_g = qg[0:2, ROWS : 2 * ROWS].reshape(2 * ROWS, HD)
    block = ck_ref.shape[0]
    cand_token = lax.broadcasted_iota(jnp.int32, (block, 2 * ROWS), 0)
    allowed = (sample_of(cand_token) == sample) & (cand_token <= token)
    score = lax.dot_general(ck_ref[...], own_q, NT, preferred_element_type=F32) * SCORE
    score = jnp.where(allowed, score, NEG)
    own_high = jnp.max(score, axis=0, keepdims=True)
    expon = jnp.exp2(score - own_high)
    product = lax.dot_general(cv_ref[...], own_g, NT, preferred_element_type=F32)
    own_total = jnp.sum(expon, axis=0, keepdims=True)
    own_carry = jnp.sum(expon * product, axis=0, keepdims=True)
    self_e[...] = expon
    self_p[...] = product

    def first_key(place):
        behind = lax.rem(z + NZ - BACK[place], NZ)
        return (((behind * 2 + xh) * 2 + core) * 8 + y * 2 + xl) * KEYS

    starts = [first_key(place).astype(F32) for place in range(NZ)]

    def first_pass(t, groups):
        rows_q = qg[pl.ds(4 * t, 4), 0:ROWS].reshape(TILE, HD)
        rows_g = qg[pl.ds(4 * t, 4), ROWS : 2 * ROWS].reshape(TILE, HD)
        coded = [qg[4 * t + 2 * i, 2 * ROWS : PIECE].astype(F32) for i in range(2)]
        rows_limit = jnp.concatenate([c[0:1] * 256.0 + c[8:9] for c in coded], axis=1)
        for g in groups:
            low, high = GROUPS[g]
            count = (high - low) * KEYS
            keys = kv[0, low:high].reshape(count, HD)
            values = kv[1, low:high].reshape(count, HD)
            score = lax.dot_general(keys, rows_q, NT, preferred_element_type=F32) * SCORE
            index = lax.broadcasted_iota(jnp.int32, (KEYS, TILE), 0).astype(F32)
            masked = []
            for i, place in enumerate(range(low, high)):
                seen = index < rows_limit - starts[place]
                masked.append(jnp.where(seen, score[i * KEYS : (i + 1) * KEYS], NEG))
            score = jnp.concatenate(masked, axis=0)
            top = jnp.max(score, axis=0, keepdims=True)
            expon = jnp.exp2(score - top)
            product = lax.dot_general(values, rows_g, NT, preferred_element_type=F32)
            e_buf[t, low * KEYS : high * KEYS] = expon
            p_buf[t, low * KEYS : high * KEYS] = product
            mg[t, g : g + 1] = top
            tot[t, g : g + 1] = jnp.sum(expon, axis=0, keepdims=True)
            car[t, g : g + 1] = jnp.sum(expon * product, axis=0, keepdims=True)

    def run_first_pass(start, stop, groups):
        def step(t, carry):
            first_pass(t, groups)
            return carry

        lax.fori_loop(start, stop, step, 0)

    def close_rows(t, carry):
        highs = mg[t]
        top = jnp.max(highs, axis=0, keepdims=True)
        weight = jnp.exp2(highs - top)
        total = jnp.sum(tot[t] * weight, axis=0, keepdims=True)
        carried = jnp.sum(car[t] * weight, axis=0, keepdims=True)
        stats = jnp.concatenate([top, total, carried, top], axis=0)
        stat_out[2 * t] = stats[:, : 2 * ROWS]
        stat_out[2 * t + 1] = stats[:, 2 * ROWS :]
        return carry

    def tile_wait(tiles):
        for t in tiles:
            for r in (2 * t, 2 * t + 1):
                if not (isinstance(r, int) and r == 0):
                    rows_wait(2 * r + other)

    for k in (1, 2, 3):
        rows_from(k, 0)
    kv_wait(0, 2)
    kv_to(0, 2, 4, up2)
    kv_to(0, 2, 3, up)
    kv_wait(0, 6)
    kv_to(0, 6, 5, down)
    kv_wait(1, 6)
    kv_to(1, 6, 4, down2)
    kv_to(1, 6, 5, down)
    kv_wait(1, 2)
    kv_to(1, 2, 3, up)
    for k in (1, 2, 3):
        rows_from(0, k)
    for kind in range(2):
        for back in (1, 7):
            kv_wait(kind, back)
    tile_wait((0, 1, 2))
    run_first_pass(0, 3, (0, 1))
    for first, second in ((1, 1), (2, 1), (1, 2), (2, 2)):
        rows_from(first, second)
    for kind in range(2):
        for back in (3, 5, 4):
            kv_wait(kind, back)
    run_first_pass(0, 3, (2,))
    for first, second in ((3, 1), (3, 2), (1, 3), (2, 3), (3, 3)):
        rows_from(first, second)

    def last_tiles(t, carry):
        tile_wait((t,))
        first_pass(t, (0, 1, 2))
        return carry

    lax.fori_loop(3, TILES, last_tiles, 0)
    lax.fori_loop(0, TILES, close_rows, 0)

    send(stat_out, stat_mate, mate_send, mate_recv, mate)
    for r in FARTHEST:
        slot = 2 * SEEN[r] + core
        send(
            stat_out.at[r], stat_in.at[slot], st_send.at[r], st_recv.at[slot],
            {**chips[r], "core": 1},
        )

    for place in range(NZ):
        kt[:, place * KEYS : (place + 1) * KEYS] = kv[0, place].astype(F32).T.astype(BF16)

    arrived(stat_mate, mate_send, mate_recv)

    def query_products(t, carry):
        pair = [
            jnp.concatenate([ref[2 * t], ref[2 * t + 1]], axis=1) for ref in (stat_out, stat_mate)
        ]
        top = jnp.maximum(pair[0][0:1], pair[1][0:1])
        scaled = [part_of * jnp.exp2(part_of[0:1] - top) for part_of in pair]
        delta = (scaled[0][2:3] + scaled[1][2:3]) / (scaled[0][1:2] + scaled[1][1:2])
        loc[t] = jnp.concatenate([top, delta], axis=0)
        expons, slopes = [], []
        for g, (low, high) in enumerate(GROUPS):
            weight = jnp.exp2(mg[t, g : g + 1] - top)
            expon = e_buf[t, low * KEYS : high * KEYS] * weight
            expons.append(expon.astype(BF16))
            slopes.append((expon * (p_buf[t, low * KEYS : high * KEYS] - delta)).astype(BF16))
        for i, right in enumerate((slopes, expons)):
            ab[t, i] = jnp.dot(kt[...], jnp.concatenate(right, axis=0), preferred_element_type=F32)
        remote(ab.at[t], ab_mate.at[t], ab_send.at[t], ab_recv.at[t], mate).start()
        return carry

    lax.fori_loop(0, TILES, query_products, 0)

    def final_sends():
        copies = []
        for r in FARTHEST:
            for c in (0, 1):
                copies.append(
                    remote(
                        fin_out, fin.at[SEEN[r]], fin_send.at[2 * r + c], fin_recv.at[SEEN[r]],
                        {**chips[r], "core": c},
                    )
                )
        copies.append(remote(fin_out, fin.at[0], fin_send.at[0], fin_recv.at[0], {"core": 0}))
        return copies

    @pl.when(core == 1)
    def _():
        for r in NEAREST:
            for c in range(2):
                arrived(stat_in.at[2 * r + c], st_send.at[1], st_recv.at[2 * r + c])
        stat_in[0] = stat_mate[0]
        stat_in[1] = stat_out[0]
        top = own_high
        for i in range(PEERS):
            top = jnp.maximum(top, stat_in[i][0:1])
        weight = jnp.exp2(own_high - top)
        total, carried = own_total * weight, own_carry * weight
        for i in range(PEERS):
            stats = stat_in[i]
            weight = jnp.exp2(stats[0:1] - top)
            total += stats[1:2] * weight
            carried += stats[2:3] * weight
        inverse = 1.0 / total
        final = jnp.concatenate([top, inverse, carried * inverse, top], axis=0)
        fin_out[...] = final
        fin[0] = final
        for copy in final_sends():
            copy.start()

    @pl.when(core == 0)
    def _():
        arrived(fin.at[0], fin_send.at[0], fin_recv.at[0])

    for t in range(TILES):
        remote(ab.at[t], ab_mate.at[t], ab_send.at[t], ab_recv.at[t], mate).wait()
    for r in NEAREST:
        arrived(fin.at[r], fin_send.at[1], fin_recv.at[r])

    def close_weights(t, carry):
        final = jnp.concatenate([fin[2 * t], fin[2 * t + 1]], axis=1)
        mg[t] = jnp.exp2(mg[t] - final[0:1]) * final[1:2]
        return carry

    lax.fori_loop(0, TILES, close_weights, 0)

    def second_pass(place, carry):
        g = lax.div(place + 1, 3)
        grad_k = jnp.zeros((KEYS, HD), F32)
        grad_v = jnp.zeros((KEYS, HD), F32)
        for t in range(TILES):
            delta = jnp.concatenate([fin[2 * t, 2:3], fin[2 * t + 1, 2:3]], axis=1)
            at = pl.ds(pl.multiple_of(place * KEYS, KEYS), KEYS)
            probs = e_buf[t, at] * mg[t, pl.ds(g, 1)]
            slopes = (probs * (p_buf[t, at] - delta)).astype(BF16)
            rows_q = qg[4 * t : 4 * t + 4, 0:ROWS].reshape(TILE, HD)
            rows_g = qg[4 * t : 4 * t + 4, ROWS : 2 * ROWS].reshape(TILE, HD)
            grad_v += jnp.dot(probs.astype(BF16), rows_g, preferred_element_type=F32)
            grad_k += jnp.dot(slopes, rows_q, preferred_element_type=F32)
        part[place, 0] = grad_k * SCALING
        part[place, 1] = grad_v
        return carry

    def pass_on(kind, back, dst, sem, device, *more):
        at = PLACE[back]
        total = part[at, kind]
        for ref in more:
            total = total + ref[...].astype(F32)
        rs_out[kind, at] = total.astype(BF16)
        send(rs_out.at[kind, at], dst, rs_send.at[kind, at], sem, device)

    second_pass(PLACE[4], 0)
    pass_on(0, 4, rs_far.at[0], far_recv.at[0], down2)
    pass_on(1, 4, rs_far.at[1], far_recv.at[1], up2)
    second_pass(PLACE[3], 0)
    for kind in range(2):
        pass_on(kind, 3, rs_near.at[kind, 0], near_recv.at[kind, 0], down)
    second_pass(PLACE[5], 0)
    for kind in range(2):
        pass_on(kind, 5, rs_near.at[kind, 1], near_recv.at[kind, 1], up)

    def query_pass(t, carry):
        final = jnp.concatenate([fin[2 * t], fin[2 * t + 1]], axis=1)
        weight = jnp.exp2(loc[t, 0:1] - final[0:1]) * final[1:2] * SCALING
        slopes, expons = (ab[t, i] + ab_mate[t, i] for i in range(2))
        grads = (slopes - expons * (final[2:3] - loc[t, 1:2])) * weight
        rows = grads.T.astype(BF16)
        for i in range(2):
            for c in range(2):
                at = (2 * i + c) * ROWS
                dq_out[c, 2 * t + i] = rows[at : at + ROWS]
        return carry

    lax.fori_loop(0, TILES, query_pass, 0)
    for r in FARTHEST:
        send(dq_out.at[core, r], dq_in.at[SEEN[r]], dq_send.at[r], dq_recv.at[SEEN[r]], chips[r])
    lax.fori_loop(0, 2, lambda i, c: second_pass(2 - i, c), 0)
    for kind in range(2):
        pass_on(kind, 7, rs_end.at[kind, 2], end_recv.at[kind, 2], up)
        pass_on(kind, 1, rs_end.at[kind, 0], end_recv.at[kind, 0], down)
    lax.fori_loop(0, 2, lambda i, c: second_pass(4 - i, c), 0)

    def two_on(kind, way):
        arrived(rs_near.at[kind, way], rs_send.at[kind, 0], near_recv.at[kind, way])
        more = [rs_near.at[kind, way]]
        if kind == way:
            arrived(rs_far.at[way], rs_send.at[kind, 0], far_recv.at[way])
            more.append(rs_far.at[way])
        slot = 1 + 2 * way
        device = (down2, up2)[way]
        pass_on(
            kind, (2, 6)[way], rs_end.at[kind, slot], end_recv.at[kind, slot], device, *more
        )

    final = fin[0]
    self_probs = self_e[...] * (jnp.exp2(own_high - final[0:1]) * final[1:2])
    self_slopes = (self_probs * (self_p[...] - final[2:3])).astype(BF16)
    self_keys = ck_ref[...].astype(F32).T.astype(BF16)
    dq_self[...] = (jnp.dot(self_keys, self_slopes, preferred_element_type=F32) * SCALING).T
    for kind, way in ((1, 0), (0, 1), (0, 0), (1, 1)):
        two_on(kind, way)
    second_pass(0, 0)

    grads = dq_self[pl.ds(pl.multiple_of(core * ROWS, ROWS), ROWS)] + dq_out[core, 0].astype(F32)
    for r in NEAREST:
        arrived(dq_in.at[r], dq_send.at[1], dq_recv.at[r])
        grads += dq_in[r].astype(F32)
    gq_ref[...] = jnp.concatenate(
        [grads[h * TOK : (h + 1) * TOK] for h in range(HEADS)], axis=1
    ).astype(BF16)
    for kind, out in enumerate((gk_ref, gv_ref)):
        total = part[0, kind]
        for way in (0, 2, 1, 3):
            arrived(rs_end.at[kind, way], rs_send.at[kind, 0], end_recv.at[kind, way])
            total = total + rs_end[kind, way].astype(F32)
        out[...] = total.astype(BF16)
    for copy in sent:
        copy.wait_send()

    @pl.when(core == 1)
    def _():
        for copy in final_sends():
            copy.wait_send()


def store(*refs):
    sems = refs[6]
    copies = [pltpu.make_async_copy(refs[i], refs[3 + i], sems.at[i]) for i in range(3)]
    for copy in copies:
        copy.start()
    for copy in copies:
        copy.wait()


def body(queries, grad_out, prefix_keys, prefix_values, cand_keys, cand_values, lengths, offsets):
    vmem = pl.BlockSpec(memory_space=pltpu.VMEM)
    anywhere = pl.BlockSpec(memory_space=pl.ANY)
    keys = NZ * KEYS
    block = cand_keys.shape[0]
    sem = pltpu.SemaphoreType.DMA
    found = pl.pallas_call(
        kernel,
        out_shape=(
            pltpu.VMEM(queries.shape, BF16),
            pltpu.VMEM(prefix_keys.shape, BF16),
            pltpu.VMEM(prefix_values.shape, BF16),
        ),
        in_specs=[anywhere] * 8,
        out_specs=(vmem,) * 3,
        scratch_shapes=[
            pltpu.VMEM(queries.shape, BF16),
            pltpu.VMEM(grad_out.shape, BF16),
            pltpu.VMEM(cand_keys.shape, BF16),
            pltpu.VMEM(cand_values.shape, BF16),
            pltpu.SMEM(lengths.shape, jnp.int32),
            pltpu.SMEM(offsets.shape, jnp.int32),
            sem((8,)),
            pltpu.VMEM((PEERS, PIECE, HD), BF16),
            pltpu.VMEM((2, NZ, KEYS, HD), BF16),
            pltpu.VMEM((HD, keys), BF16),
            pltpu.VMEM((TILES, keys, TILE), F32),
            pltpu.VMEM((TILES, keys, TILE), F32),
            pltpu.VMEM((TILES, len(GROUPS), TILE), F32),
            pltpu.VMEM((TILES, len(GROUPS), TILE), F32),
            pltpu.VMEM((TILES, len(GROUPS), TILE), F32),
            pltpu.VMEM((TILES, 2, TILE), F32),
            pltpu.VMEM((TILES, 2, HD, TILE), F32),
            pltpu.VMEM((TILES, 2, HD, TILE), F32),
            pltpu.VMEM((CHIPS, 4, 2 * ROWS), F32),
            pltpu.VMEM((PEERS, 4, 2 * ROWS), F32),
            pltpu.VMEM((CHIPS, 4, 2 * ROWS), F32),
            pltpu.VMEM((4, 2 * ROWS), F32),
            pltpu.VMEM((CHIPS, 4, 2 * ROWS), F32),
            pltpu.VMEM((block, 2 * ROWS), F32),
            pltpu.VMEM((block, 2 * ROWS), F32),
            pltpu.VMEM((2, CHIPS, ROWS, HD), BF16),
            pltpu.VMEM((CHIPS, ROWS, HD), BF16),
            pltpu.VMEM((2 * ROWS, HD), F32),
            pltpu.VMEM((NZ, 2, KEYS, HD), F32),
            pltpu.VMEM((2, NZ, KEYS, HD), BF16),
            pltpu.VMEM((2, 2, KEYS, HD), BF16),
            pltpu.VMEM((2, KEYS, HD), BF16),
            pltpu.VMEM((2, 4, KEYS, HD), BF16),
            sem((PEERS,)),
            sem((PEERS,)),
            sem((2, NZ)),
            sem((2, NZ)),
            sem((CHIPS,)),
            sem((PEERS,)),
            sem((PEERS,)),
            sem((CHIPS,)),
            sem,
            sem,
            sem((TILES,)),
            sem((TILES,)),
            sem((CHIPS,)),
            sem((CHIPS,)),
            sem((2, NZ)),
            sem((2, 2)),
            sem((2,)),
            sem((2, 4)),
        ],
        compiler_params=pltpu.CompilerParams(
            collective_id=0, has_side_effects=True, vmem_limit_bytes=56 * 1024 * 1024
        ),
        name="attention_grads",
    )(queries, grad_out, prefix_keys, prefix_values, cand_keys, cand_values, lengths, offsets)
    return pl.pallas_call(
        store,
        out_shape=tuple(jax.ShapeDtypeStruct(a.shape, BF16) for a in found),
        in_specs=[vmem] * 3,
        out_specs=(anywhere,) * 3,
        scratch_shapes=[sem((3,))],
        name="store",
    )(*(pltpu.with_memory_space_constraint(a, pltpu.VMEM) for a in found))


def solution(mesh):
    torus = Mesh(mesh.devices.reshape(NZ, 2, 2, NY, 2), AXES)
    in_specs = (
        P(CAND_CTX, None),
        P(CAND_CTX, None),
        P(CTX_CAND, None),
        P(CTX_CAND, None),
        P(CAND, None),
        P(CAND, None),
        P(CAND, None),
        P(CAND),
    )
    out_specs = (P(CAND_CTX, None), P(CTX_CAND, None), P(CTX_CAND, None))
    return jax.shard_map(body, mesh=torus, in_specs=in_specs, out_specs=out_specs, check_vma=False)
```

```python
import math

import jax
import jax.numpy as jnp
from jax import lax
from jax.experimental import pallas as pl
from jax.experimental.pallas import tpu as pltpu
from jax.sharding import Mesh
from jax.sharding import PartitionSpec as P

HEADS = 8
HD = 128
NX = NY = 4
NZ = 8
CHIPS = NX * NY
PEERS = 2 * CHIPS
TOK = 8
ROWS = TOK * HEADS
TILE = 4 * ROWS
TILES = PEERS * ROWS // TILE
KEYS = 128
GROUPS = ((0, 2), (2, 5), (5, 8))
SAMPLES = 4
AXES = ("z", "xh", "core", "y", "xl")
CAND = ("y", "xl")
CAND_CTX = ("y", "xl", "z", "xh", "core")
CTX_CAND = ("z", "xh", "core", "y", "xl")
MESH = pl.DeviceIdType.MESH
NEG = -1e30
SCALING = 1.0 / math.sqrt(HD)
SCORE = SCALING * math.log2(math.e)
PLACE = {0: 0, 1: 1, 7: 2, 2: 3, 6: 4, 3: 5, 5: 6, 4: 7}
BACK = {place: r for r, place in PLACE.items()}
STEPS = (0, 1, 3, 2)
BACKWARD = (0, 2, 1, 3)
HOPS = (0, 1, 1, 2)
ORDER = (
    (0, 0), (0, 1), (1, 0), (0, 2), (2, 0), (0, 3), (3, 0), (1, 1),
    (2, 1), (1, 2), (2, 2), (1, 3), (3, 1), (2, 3), (3, 2), (3, 3),
)
FAR = [HOPS[a] + HOPS[b] for a, b in ORDER]
SEEN = [ORDER.index((BACKWARD[a], BACKWARD[b])) for a, b in ORDER]
NEAREST = sorted(range(1, CHIPS), key=lambda r: FAR[r])
FARTHEST = NEAREST[::-1]
PIECE = 2 * ROWS + 16
F32 = jnp.float32
BF16 = jnp.bfloat16
NT = (((1,), (1,)), ((), ()))


def stacked(block):
    wide = block.astype(F32)
    return jnp.concatenate([wide[:, h * HD : (h + 1) * HD] for h in range(HEADS)], axis=0)


def kernel(
    q_hbm, g_hbm, pk_hbm, pv_hbm, ck_hbm, cv_hbm, len_hbm, off_hbm,
    gq_ref, gk_ref, gv_ref,
    q_ref, g_ref, ck_ref, cv_ref, len_ref, off_ref, in_sem, qg, kv, kt, e_buf, p_buf, mg, tot, car, loc, ab, ab_mate, stat_out, stat_in, stat_mate, fin_out, fin,
    self_e, self_p, dq_out, dq_in, dq_self, part, rs_out, rs_near, rs_far, rs_end,
    qg_send, qg_recv, kv_send, kv_recv,
    st_send, st_recv, fin_send, fin_recv, mate_send, mate_recv, ab_send, ab_recv, dq_send, dq_recv,
    rs_send, near_recv, far_recv, end_recv,
):
    z, xh, core, y, xl = (lax.axis_index(a) for a in AXES)
    x = 2 * xh + xl
    other = 1 - core
    mate = {"core": other}
    up, up2, down2, down = ({"z": lax.rem(z + d, NZ)} for d in (1, 2, NZ - 2, NZ - 1))
    chips = []
    for r in range(CHIPS):
        px, py = lax.rem(x + STEPS[ORDER[r][0]], NX), lax.rem(y + STEPS[ORDER[r][1]], NY)
        chips.append({"xh": lax.div(px, 2), "xl": lax.rem(px, 2), "y": py})

    def along(axis, k):
        px = lax.rem(x + STEPS[k] * (core if axis == 0 else other), NX)
        py = lax.rem(y + STEPS[k] * (other if axis == 0 else core), NY)
        return {"xh": lax.div(px, 2), "xl": lax.rem(px, 2), "y": py}

    lines = [[along(axis, k) for k in range(4)] for axis in range(2)]
    sent = []

    def remote(src, dst, send_sem, recv_sem, device):
        return pltpu.make_async_remote_copy(
            src_ref=src, dst_ref=dst, send_sem=send_sem, recv_sem=recv_sem,
            device_id=device, device_id_type=MESH,
        )

    def send(*args):
        copy = remote(*args)
        copy.start()
        sent.append(copy)

    def arrived(dst, send_sem, recv_sem):
        remote(dst, dst, send_sem, recv_sem, mate).wait_recv()

    inputs = [
        pltpu.make_async_copy(src, dst, in_sem.at[i])
        for i, (src, dst) in enumerate(
            (
                (pk_hbm, kv.at[0, 0]), (pv_hbm, kv.at[1, 0]), (q_hbm, q_ref), (g_hbm, g_ref),
                (len_hbm, len_ref), (off_hbm, off_ref), (ck_hbm, ck_ref), (cv_hbm, cv_ref),
            )
        )
    ]
    for copy in inputs:
        copy.start()
    barrier = pltpu.get_barrier_semaphore()
    greeted = [mate, up, down, up2, down2] + lines[0][1:] + lines[1][1:]
    for device in greeted:
        pl.semaphore_signal(barrier, inc=1, device_id=device, device_id_type=MESH)
    for copy in inputs[2:6]:
        copy.wait()

    qg[core, 0:ROWS] = stacked(q_ref[...]).astype(BF16)
    qg[core, ROWS : 2 * ROWS] = stacked(g_ref[...]).astype(BF16)

    ends = [len_ref[0, 0]]
    for s in range(1, SAMPLES):
        ends.append(ends[-1] + len_ref[0, s])

    def sample_of(token):
        return sum((token >= end).astype(jnp.int32) for end in ends)

    lane = lax.broadcasted_iota(jnp.int32, (1, 2 * ROWS), 1)
    token = ((z * 2 + xh) * 2 + lax.div(lane, ROWS)) * TOK + lax.rem(lane, TOK)
    sample = sample_of(token)
    high, low = jnp.zeros((1, 2 * ROWS), F32), jnp.zeros((1, 2 * ROWS), F32)
    for s in range(SAMPLES):
        mine = sample == s
        high = jnp.where(mine, lax.div(off_ref[s], 256).astype(F32), high)
        low = jnp.where(mine, lax.rem(off_ref[s], 256).astype(F32), low)
    high, low = (jnp.broadcast_to(part_of, (8, 2 * ROWS)) for part_of in (high, low))
    qg[core, 2 * ROWS : PIECE] = jnp.concatenate([high, low], axis=0).astype(BF16)

    for copy in inputs[:2]:
        copy.wait()
    pl.semaphore_wait(barrier, len(greeted))

    def kv_to(kind, back, new_back, device):
        at = PLACE[new_back]
        send(kv.at[kind, PLACE[back]], kv.at[kind, at], kv_send.at[kind, at], kv_recv.at[kind, at], device)

    def kv_wait(kind, back):
        at = PLACE[back]
        arrived(kv.at[kind, at], kv_send.at[kind, at], kv_recv.at[kind, at])

    def rows_wait(slot):
        arrived(qg.at[slot], qg_send.at[0], qg_recv.at[slot])

    def slot_of(first, second):
        return 2 * (other * ORDER.index((second, first)) + core * ORDER.index((first, second))) + core

    rows_sent = iter(range(PEERS))

    def rows_to(slot, there, device):
        send(qg.at[slot], qg.at[there], qg_send.at[next(rows_sent)], qg_recv.at[there], device)

    def second_line(first):
        for k in (3, 1, 2):
            rows_to(slot_of(first, 0), slot_of(first, BACKWARD[k]), lines[1][k])

    def rows_from(first, second):
        slot = slot_of(first, second)
        rows_wait(slot)
        if first and not second:
            second_line(first)
        rows_to(slot, slot, mate)

    for kind in range(2):
        kv_to(kind, 0, 2, up2)
        kv_to(kind, 0, 6, down2)
    for k in (3, 1, 2):
        rows_to(core, slot_of(BACKWARD[k], 0), lines[0][k])
    rows_to(core, core, mate)
    second_line(0)
    for kind in range(2):
        kv_to(kind, 0, 1, up)
        kv_to(kind, 0, 7, down)

    for copy in inputs[6:]:
        copy.wait()
    rows_wait(other)
    own_q = qg[0:2, 0:ROWS].reshape(2 * ROWS, HD)
    own_g = qg[0:2, ROWS : 2 * ROWS].reshape(2 * ROWS, HD)
    block = ck_ref.shape[0]
    cand_token = lax.broadcasted_iota(jnp.int32, (block, 2 * ROWS), 0)
    allowed = (sample_of(cand_token) == sample) & (cand_token <= token)
    score = lax.dot_general(ck_ref[...], own_q, NT, preferred_element_type=F32) * SCORE
    score = jnp.where(allowed, score, NEG)
    own_high = jnp.max(score, axis=0, keepdims=True)
    expon = jnp.exp2(score - own_high)
    product = lax.dot_general(cv_ref[...], own_g, NT, preferred_element_type=F32)
    own_total = jnp.sum(expon, axis=0, keepdims=True)
    own_carry = jnp.sum(expon * product, axis=0, keepdims=True)
    self_e[...] = expon
    self_p[...] = product

    def first_key(place):
        behind = lax.rem(z + NZ - BACK[place], NZ)
        return (((behind * 2 + xh) * 2 + core) * 8 + y * 2 + xl) * KEYS

    starts = [first_key(place).astype(F32) for place in range(NZ)]

    def first_pass(t, groups):
        rows_q = qg[pl.ds(4 * t, 4), 0:ROWS].reshape(TILE, HD)
        rows_g = qg[pl.ds(4 * t, 4), ROWS : 2 * ROWS].reshape(TILE, HD)
        coded = [qg[4 * t + 2 * i, 2 * ROWS : PIECE].astype(F32) for i in range(2)]
        rows_limit = jnp.concatenate([c[0:1] * 256.0 + c[8:9] for c in coded], axis=1)
        for g in groups:
            low, high = GROUPS[g]
            count = (high - low) * KEYS
            keys = kv[0, low:high].reshape(count, HD)
            values = kv[1, low:high].reshape(count, HD)
            score = lax.dot_general(keys, rows_q, NT, preferred_element_type=F32) * SCORE
            index = lax.broadcasted_iota(jnp.int32, (KEYS, TILE), 0).astype(F32)
            masked = []
            for i, place in enumerate(range(low, high)):
                seen = index < rows_limit - starts[place]
                masked.append(jnp.where(seen, score[i * KEYS : (i + 1) * KEYS], NEG))
            score = jnp.concatenate(masked, axis=0)
            top = jnp.max(score, axis=0, keepdims=True)
            expon = jnp.exp2(score - top)
            product = lax.dot_general(values, rows_g, NT, preferred_element_type=F32)
            e_buf[t, low * KEYS : high * KEYS] = expon
            p_buf[t, low * KEYS : high * KEYS] = product
            mg[t, g : g + 1] = top
            tot[t, g : g + 1] = jnp.sum(expon, axis=0, keepdims=True)
            car[t, g : g + 1] = jnp.sum(expon * product, axis=0, keepdims=True)

    def run_first_pass(start, stop, groups):
        def step(t, carry):
            first_pass(t, groups)
            return carry

        lax.fori_loop(start, stop, step, 0)

    def close_rows(t, carry):
        highs = mg[t]
        top = jnp.max(highs, axis=0, keepdims=True)
        weight = jnp.exp2(highs - top)
        total = jnp.sum(tot[t] * weight, axis=0, keepdims=True)
        carried = jnp.sum(car[t] * weight, axis=0, keepdims=True)
        stats = jnp.concatenate([top, total, carried, top], axis=0)
        stat_out[2 * t] = stats[:, : 2 * ROWS]
        stat_out[2 * t + 1] = stats[:, 2 * ROWS :]
        return carry

    def tile_wait(tiles):
        for t in tiles:
            for r in (2 * t, 2 * t + 1):
                if not (isinstance(r, int) and r == 0):
                    rows_wait(2 * r + other)

    for k in (1, 2, 3):
        rows_from(k, 0)
    kv_wait(0, 2)
    kv_to(0, 2, 4, up2)
    kv_to(0, 2, 3, up)
    kv_wait(0, 6)
    kv_to(0, 6, 5, down)
    kv_wait(1, 6)
    kv_to(1, 6, 4, down2)
    kv_to(1, 6, 5, down)
    kv_wait(1, 2)
    kv_to(1, 2, 3, up)
    for k in (1, 2, 3):
        rows_from(0, k)
    for kind in range(2):
        for back in (1, 7):
            kv_wait(kind, back)
    tile_wait((0, 1, 2))
    run_first_pass(0, 3, (0, 1))
    for first, second in ((1, 1), (2, 1), (1, 2), (2, 2)):
        rows_from(first, second)
    for kind in range(2):
        for back in (3, 5, 4):
            kv_wait(kind, back)
    run_first_pass(0, 3, (2,))
    lax.fori_loop(0, 3, close_rows, 0)
    for first, second in ((3, 1), (3, 2), (1, 3), (2, 3), (3, 3)):
        rows_from(first, second)

    def last_tiles(t, carry):
        tile_wait((t,))
        first_pass(t, (0, 1, 2))
        return close_rows(t, carry)

    lax.fori_loop(3, TILES, last_tiles, 0)

    send(stat_out, stat_mate, mate_send, mate_recv, mate)
    for r in FARTHEST:
        slot = 2 * SEEN[r] + core
        send(
            stat_out.at[r], stat_in.at[slot], st_send.at[r], st_recv.at[slot],
            {**chips[r], "core": 1},
        )

    for place in range(NZ):
        kt[:, place * KEYS : (place + 1) * KEYS] = kv[0, place].astype(F32).T.astype(BF16)

    arrived(stat_mate, mate_send, mate_recv)

    def query_products(t, carry):
        pair = [
            jnp.concatenate([ref[2 * t], ref[2 * t + 1]], axis=1) for ref in (stat_out, stat_mate)
        ]
        top = jnp.maximum(pair[0][0:1], pair[1][0:1])
        scaled = [part_of * jnp.exp2(part_of[0:1] - top) for part_of in pair]
        delta = (scaled[0][2:3] + scaled[1][2:3]) / (scaled[0][1:2] + scaled[1][1:2])
        loc[t] = jnp.concatenate([top, delta], axis=0)
        expons, slopes = [], []
        for g, (low, high) in enumerate(GROUPS):
            weight = jnp.exp2(mg[t, g : g + 1] - top)
            expon = e_buf[t, low * KEYS : high * KEYS] * weight
            expons.append(expon.astype(BF16))
            slopes.append((expon * (p_buf[t, low * KEYS : high * KEYS] - delta)).astype(BF16))
        for i, right in enumerate((slopes, expons)):
            ab[t, i] = jnp.dot(kt[...], jnp.concatenate(right, axis=0), preferred_element_type=F32)
        remote(ab.at[t], ab_mate.at[t], ab_send.at[t], ab_recv.at[t], mate).start()
        return carry

    lax.fori_loop(0, TILES, query_products, 0)

    def final_sends():
        copies = []
        for r in FARTHEST:
            for c in (0, 1):
                copies.append(
                    remote(
                        fin_out, fin.at[SEEN[r]], fin_send.at[2 * r + c], fin_recv.at[SEEN[r]],
                        {**chips[r], "core": c},
                    )
                )
        copies.append(remote(fin_out, fin.at[0], fin_send.at[0], fin_recv.at[0], {"core": 0}))
        return copies

    @pl.when(core == 1)
    def _():
        for r in NEAREST:
            for c in range(2):
                arrived(stat_in.at[2 * r + c], st_send.at[1], st_recv.at[2 * r + c])
        stat_in[0] = stat_mate[0]
        stat_in[1] = stat_out[0]
        top = own_high
        for i in range(PEERS):
            top = jnp.maximum(top, stat_in[i][0:1])
        weight = jnp.exp2(own_high - top)
        total, carried = own_total * weight, own_carry * weight
        for i in range(PEERS):
            stats = stat_in[i]
            weight = jnp.exp2(stats[0:1] - top)
            total += stats[1:2] * weight
            carried += stats[2:3] * weight
        inverse = 1.0 / total
        final = jnp.concatenate([top, inverse, carried * inverse, top], axis=0)
        fin_out[...] = final
        fin[0] = final
        for copy in final_sends():
            copy.start()

    @pl.when(core == 0)
    def _():
        arrived(fin.at[0], fin_send.at[0], fin_recv.at[0])

    def final_wait(chips_there):
        for r in chips_there:
            arrived(fin.at[r], fin_send.at[1], fin_recv.at[r])

    def close_weights(t, carry):
        final = jnp.concatenate([fin[2 * t], fin[2 * t + 1]], axis=1)
        mg[t] = jnp.exp2(mg[t] - final[0:1]) * final[1:2]
        return carry


    def second_pass(place, carry, tiles=range(TILES), more=False):
        g = lax.div(place + 1, 3)
        grad_k = jnp.zeros((KEYS, HD), F32)
        grad_v = jnp.zeros((KEYS, HD), F32)
        for t in tiles:
            delta = jnp.concatenate([fin[2 * t, 2:3], fin[2 * t + 1, 2:3]], axis=1)
            at = pl.ds(pl.multiple_of(place * KEYS, KEYS), KEYS)
            probs = e_buf[t, at] * mg[t, pl.ds(g, 1)]
            slopes = (probs * (p_buf[t, at] - delta)).astype(BF16)
            rows_q = qg[4 * t : 4 * t + 4, 0:ROWS].reshape(TILE, HD)
            rows_g = qg[4 * t : 4 * t + 4, ROWS : 2 * ROWS].reshape(TILE, HD)
            grad_v += jnp.dot(probs.astype(BF16), rows_g, preferred_element_type=F32)
            grad_k += jnp.dot(slopes, rows_q, preferred_element_type=F32)
        grad_k = grad_k * SCALING
        part[place, 0] = part[place, 0] + grad_k if more else grad_k
        part[place, 1] = part[place, 1] + grad_v if more else grad_v
        return carry

    def pass_on(kind, back, dst, sem, device, *more):
        at = PLACE[back]
        total = part[at, kind]
        for ref in more:
            total = total + ref[...].astype(F32)
        rs_out[kind, at] = total.astype(BF16)
        send(rs_out.at[kind, at], dst, rs_send.at[kind, at], sem, device)

    near_tiles, far_tiles = range(TILES // 2), range(TILES // 2, TILES)
    final_wait(range(1, CHIPS // 2))
    lax.fori_loop(0, TILES // 2, close_weights, 0)
    lax.fori_loop(0, 3, lambda i, c: second_pass(7 - i, c, near_tiles), 0)
    final_wait(range(CHIPS // 2, CHIPS))
    lax.fori_loop(TILES // 2, TILES, close_weights, 0)
    second_pass(PLACE[4], 0, far_tiles, True)
    pass_on(0, 4, rs_far.at[0], far_recv.at[0], down2)
    pass_on(1, 4, rs_far.at[1], far_recv.at[1], up2)
    second_pass(PLACE[3], 0, far_tiles, True)
    for kind in range(2):
        pass_on(kind, 3, rs_near.at[kind, 0], near_recv.at[kind, 0], down)
    second_pass(PLACE[5], 0, far_tiles, True)
    for kind in range(2):
        pass_on(kind, 5, rs_near.at[kind, 1], near_recv.at[kind, 1], up)

    def query_pass(t, carry):
        final = jnp.concatenate([fin[2 * t], fin[2 * t + 1]], axis=1)
        weight = jnp.exp2(loc[t, 0:1] - final[0:1]) * final[1:2] * SCALING
        slopes, expons = (ab[t, i] + ab_mate[t, i] for i in range(2))
        grads = (slopes - expons * (final[2:3] - loc[t, 1:2])) * weight
        rows = grads.T.astype(BF16)
        for i in range(2):
            for c in range(2):
                at = (2 * i + c) * ROWS
                dq_out[c, 2 * t + i] = rows[at : at + ROWS]
        return carry

    for t in range(TILES):
        remote(ab.at[t], ab_mate.at[t], ab_send.at[t], ab_recv.at[t], mate).wait()
    lax.fori_loop(0, TILES, query_pass, 0)
    for r in FARTHEST:
        send(dq_out.at[core, r], dq_in.at[SEEN[r]], dq_send.at[r], dq_recv.at[SEEN[r]], chips[r])
    lax.fori_loop(0, 2, lambda i, c: second_pass(2 - i, c), 0)
    for kind in range(2):
        pass_on(kind, 7, rs_end.at[kind, 2], end_recv.at[kind, 2], up)
        pass_on(kind, 1, rs_end.at[kind, 0], end_recv.at[kind, 0], down)
    lax.fori_loop(0, 2, lambda i, c: second_pass(4 - i, c), 0)

    def two_on(kind, way):
        arrived(rs_near.at[kind, way], rs_send.at[kind, 0], near_recv.at[kind, way])
        more = [rs_near.at[kind, way]]
        if kind == way:
            arrived(rs_far.at[way], rs_send.at[kind, 0], far_recv.at[way])
            more.append(rs_far.at[way])
        slot = 1 + 2 * way
        device = (down2, up2)[way]
        pass_on(
            kind, (2, 6)[way], rs_end.at[kind, slot], end_recv.at[kind, slot], device, *more
        )

    final = fin[0]
    self_probs = self_e[...] * (jnp.exp2(own_high - final[0:1]) * final[1:2])
    self_slopes = (self_probs * (self_p[...] - final[2:3])).astype(BF16)
    self_keys = ck_ref[...].astype(F32).T.astype(BF16)
    dq_self[...] = (jnp.dot(self_keys, self_slopes, preferred_element_type=F32) * SCALING).T
    for kind, way in ((1, 0), (0, 1), (0, 0), (1, 1)):
        two_on(kind, way)
    second_pass(0, 0)

    grads = dq_self[pl.ds(pl.multiple_of(core * ROWS, ROWS), ROWS)] + dq_out[core, 0].astype(F32)
    for r in NEAREST:
        arrived(dq_in.at[r], dq_send.at[1], dq_recv.at[r])
        grads += dq_in[r].astype(F32)
    gq_ref[...] = jnp.concatenate(
        [grads[h * TOK : (h + 1) * TOK] for h in range(HEADS)], axis=1
    ).astype(BF16)
    for kind, out in enumerate((gk_ref, gv_ref)):
        total = part[0, kind]
        for way in (0, 2, 1, 3):
            arrived(rs_end.at[kind, way], rs_send.at[kind, 0], end_recv.at[kind, way])
            total = total + rs_end[kind, way].astype(F32)
        out[...] = total.astype(BF16)
    for copy in sent:
        copy.wait_send()

    @pl.when(core == 1)
    def _():
        for copy in final_sends():
            copy.wait_send()


def store(*refs):
    sems = refs[6]
    copies = [pltpu.make_async_copy(refs[i], refs[3 + i], sems.at[i]) for i in range(3)]
    for copy in copies:
        copy.start()
    for copy in copies:
        copy.wait()


def body(queries, grad_out, prefix_keys, prefix_values, cand_keys, cand_values, lengths, offsets):
    vmem = pl.BlockSpec(memory_space=pltpu.VMEM)
    anywhere = pl.BlockSpec(memory_space=pl.ANY)
    keys = NZ * KEYS
    block = cand_keys.shape[0]
    sem = pltpu.SemaphoreType.DMA
    found = pl.pallas_call(
        kernel,
        out_shape=(
            pltpu.VMEM(queries.shape, BF16),
            pltpu.VMEM(prefix_keys.shape, BF16),
            pltpu.VMEM(prefix_values.shape, BF16),
        ),
        in_specs=[anywhere] * 8,
        out_specs=(vmem,) * 3,
        scratch_shapes=[
            pltpu.VMEM(queries.shape, BF16),
            pltpu.VMEM(grad_out.shape, BF16),
            pltpu.VMEM(cand_keys.shape, BF16),
            pltpu.VMEM(cand_values.shape, BF16),
            pltpu.SMEM(lengths.shape, jnp.int32),
            pltpu.SMEM(offsets.shape, jnp.int32),
            sem((8,)),
            pltpu.VMEM((PEERS, PIECE, HD), BF16),
            pltpu.VMEM((2, NZ, KEYS, HD), BF16),
            pltpu.VMEM((HD, keys), BF16),
            pltpu.VMEM((TILES, keys, TILE), F32),
            pltpu.VMEM((TILES, keys, TILE), F32),
            pltpu.VMEM((TILES, len(GROUPS), TILE), F32),
            pltpu.VMEM((TILES, len(GROUPS), TILE), F32),
            pltpu.VMEM((TILES, len(GROUPS), TILE), F32),
            pltpu.VMEM((TILES, 2, TILE), F32),
            pltpu.VMEM((TILES, 2, HD, TILE), F32),
            pltpu.VMEM((TILES, 2, HD, TILE), F32),
            pltpu.VMEM((CHIPS, 4, 2 * ROWS), F32),
            pltpu.VMEM((PEERS, 4, 2 * ROWS), F32),
            pltpu.VMEM((CHIPS, 4, 2 * ROWS), F32),
            pltpu.VMEM((4, 2 * ROWS), F32),
            pltpu.VMEM((CHIPS, 4, 2 * ROWS), F32),
            pltpu.VMEM((block, 2 * ROWS), F32),
            pltpu.VMEM((block, 2 * ROWS), F32),
            pltpu.VMEM((2, CHIPS, ROWS, HD), BF16),
            pltpu.VMEM((CHIPS, ROWS, HD), BF16),
            pltpu.VMEM((2 * ROWS, HD), F32),
            pltpu.VMEM((NZ, 2, KEYS, HD), F32),
            pltpu.VMEM((2, NZ, KEYS, HD), BF16),
            pltpu.VMEM((2, 2, KEYS, HD), BF16),
            pltpu.VMEM((2, KEYS, HD), BF16),
            pltpu.VMEM((2, 4, KEYS, HD), BF16),
            sem((PEERS,)),
            sem((PEERS,)),
            sem((2, NZ)),
            sem((2, NZ)),
            sem((CHIPS,)),
            sem((PEERS,)),
            sem((PEERS,)),
            sem((CHIPS,)),
            sem,
            sem,
            sem((TILES,)),
            sem((TILES,)),
            sem((CHIPS,)),
            sem((CHIPS,)),
            sem((2, NZ)),
            sem((2, 2)),
            sem((2,)),
            sem((2, 4)),
        ],
        compiler_params=pltpu.CompilerParams(
            collective_id=0, has_side_effects=True, vmem_limit_bytes=56 * 1024 * 1024
        ),
        name="attention_grads",
    )(queries, grad_out, prefix_keys, prefix_values, cand_keys, cand_values, lengths, offsets)
    return pl.pallas_call(
        store,
        out_shape=tuple(jax.ShapeDtypeStruct(a.shape, BF16) for a in found),
        in_specs=[vmem] * 3,
        out_specs=(anywhere,) * 3,
        scratch_shapes=[sem((3,))],
        name="store",
    )(*(pltpu.with_memory_space_constraint(a, pltpu.VMEM) for a in found))


def solution(mesh):
    torus = Mesh(mesh.devices.reshape(NZ, 2, 2, NY, 2), AXES)
    in_specs = (
        P(CAND_CTX, None),
        P(CAND_CTX, None),
        P(CTX_CAND, None),
        P(CTX_CAND, None),
        P(CAND, None),
        P(CAND, None),
        P(CAND, None),
        P(CAND),
    )
    out_specs = (P(CAND_CTX, None), P(CTX_CAND, None), P(CTX_CAND, None))
    return jax.shard_map(body, mesh=torus, in_specs=in_specs, out_specs=out_specs, check_vma=False)
```

```python
import math

import jax
import jax.numpy as jnp
from jax import lax
from jax.experimental import pallas as pl
from jax.experimental.pallas import tpu as pltpu
from jax.sharding import Mesh
from jax.sharding import PartitionSpec as P

HEADS = 8
HD = 128
NX = NY = 4
NZ = 8
CHIPS = NX * NY
PEERS = 2 * CHIPS
TOK = 8
ROWS = TOK * HEADS
TILE = 4 * ROWS
TILES = PEERS * ROWS // TILE
KEYS = 128
GROUPS = ((0, 2), (2, 5), (5, 8))
SAMPLES = 4
AXES = ("z", "xh", "core", "y", "xl")
CAND = ("y", "xl")
CAND_CTX = ("y", "xl", "z", "xh", "core")
CTX_CAND = ("z", "xh", "core", "y", "xl")
MESH = pl.DeviceIdType.MESH
NEG = -1e30
SCALING = 1.0 / math.sqrt(HD)
SCORE = SCALING * math.log2(math.e)
PLACE = {0: 0, 1: 1, 7: 2, 2: 3, 6: 4, 3: 5, 5: 6, 4: 7}
BACK = {place: r for r, place in PLACE.items()}
STEPS = (0, 1, 3, 2)
BACKWARD = (0, 2, 1, 3)
HOPS = (0, 1, 1, 2)
ORDER = (
    (0, 0), (0, 1), (1, 0), (0, 2), (2, 0), (0, 3), (3, 0), (1, 1),
    (2, 1), (1, 2), (2, 2), (1, 3), (3, 1), (2, 3), (3, 2), (3, 3),
)
FAR = [HOPS[a] + HOPS[b] for a, b in ORDER]
SEEN = [ORDER.index((BACKWARD[a], BACKWARD[b])) for a, b in ORDER]
NEAREST = sorted(range(1, CHIPS), key=lambda r: FAR[r])
FARTHEST = NEAREST[::-1]
PIECE = 2 * ROWS + 16
F32 = jnp.float32
BF16 = jnp.bfloat16
NT = (((1,), (1,)), ((), ()))


def stacked(block):
    wide = block.astype(F32)
    return jnp.concatenate([wide[:, h * HD : (h + 1) * HD] for h in range(HEADS)], axis=0)


def kernel(
    q_hbm, g_hbm, pk_hbm, pv_hbm, ck_hbm, cv_hbm, len_hbm, off_hbm,
    gq_ref, gk_ref, gv_ref,
    q_ref, g_ref, ck_ref, cv_ref, len_ref, off_ref, in_sem, qg, kv, kt, e_buf, p_buf, mg, tot, car, loc, ab, ab_mate, stat_out, stat_in, stat_mate, fin_out, fin,
    self_e, self_p, dq_out, dq_in, dq_self, part, rs_out, rs_near, rs_far, rs_end,
    qg_send, qg_recv, kv_send, kv_recv,
    st_send, st_recv, fin_send, fin_recv, mate_send, mate_recv, ab_send, ab_recv, dq_send, dq_recv,
    rs_send, near_recv, far_recv, end_recv,
):
    z, xh, core, y, xl = (lax.axis_index(a) for a in AXES)
    x = 2 * xh + xl
    other = 1 - core
    mate = {"core": other}
    up, up2, down2, down = ({"z": lax.rem(z + d, NZ)} for d in (1, 2, NZ - 2, NZ - 1))
    chips = []
    for r in range(CHIPS):
        px, py = lax.rem(x + STEPS[ORDER[r][0]], NX), lax.rem(y + STEPS[ORDER[r][1]], NY)
        chips.append({"xh": lax.div(px, 2), "xl": lax.rem(px, 2), "y": py})

    def along(axis, k):
        px = lax.rem(x + STEPS[k] * (core if axis == 0 else other), NX)
        py = lax.rem(y + STEPS[k] * (other if axis == 0 else core), NY)
        return {"xh": lax.div(px, 2), "xl": lax.rem(px, 2), "y": py}

    lines = [[along(axis, k) for k in range(4)] for axis in range(2)]
    sent = []

    def remote(src, dst, send_sem, recv_sem, device):
        return pltpu.make_async_remote_copy(
            src_ref=src, dst_ref=dst, send_sem=send_sem, recv_sem=recv_sem,
            device_id=device, device_id_type=MESH,
        )

    def send(*args):
        copy = remote(*args)
        copy.start()
        sent.append(copy)

    def arrived(dst, send_sem, recv_sem):
        remote(dst, dst, send_sem, recv_sem, mate).wait_recv()

    inputs = [
        pltpu.make_async_copy(src, dst, in_sem.at[i])
        for i, (src, dst) in enumerate(
            (
                (pk_hbm, kv.at[0, 0]), (pv_hbm, kv.at[1, 0]), (q_hbm, q_ref), (g_hbm, g_ref),
                (len_hbm, len_ref), (off_hbm, off_ref), (ck_hbm, ck_ref), (cv_hbm, cv_ref),
            )
        )
    ]
    for copy in inputs:
        copy.start()
    barrier = pltpu.get_barrier_semaphore()
    greeted = [mate, up, down, up2, down2] + lines[0][1:] + lines[1][1:]
    for device in greeted:
        pl.semaphore_signal(barrier, inc=1, device_id=device, device_id_type=MESH)
    for copy in inputs[2:6]:
        copy.wait()

    qg[core, 0:ROWS] = stacked(q_ref[...]).astype(BF16)
    qg[core, ROWS : 2 * ROWS] = stacked(g_ref[...]).astype(BF16)

    ends = [len_ref[0, 0]]
    for s in range(1, SAMPLES):
        ends.append(ends[-1] + len_ref[0, s])

    def sample_of(token):
        return sum((token >= end).astype(jnp.int32) for end in ends)

    lane = lax.broadcasted_iota(jnp.int32, (1, 2 * ROWS), 1)
    token = ((z * 2 + xh) * 2 + lax.div(lane, ROWS)) * TOK + lax.rem(lane, TOK)
    sample = sample_of(token)
    high, low = jnp.zeros((1, 2 * ROWS), F32), jnp.zeros((1, 2 * ROWS), F32)
    for s in range(SAMPLES):
        mine = sample == s
        high = jnp.where(mine, lax.div(off_ref[s], 256).astype(F32), high)
        low = jnp.where(mine, lax.rem(off_ref[s], 256).astype(F32), low)
    high, low = (jnp.broadcast_to(part_of, (8, 2 * ROWS)) for part_of in (high, low))
    qg[core, 2 * ROWS : PIECE] = jnp.concatenate([high, low], axis=0).astype(BF16)

    for copy in inputs[:2]:
        copy.wait()
    pl.semaphore_wait(barrier, len(greeted))

    def kv_to(kind, back, new_back, device):
        at = PLACE[new_back]
        send(kv.at[kind, PLACE[back]], kv.at[kind, at], kv_send.at[kind, at], kv_recv.at[kind, at], device)

    def kv_wait(kind, back):
        at = PLACE[back]
        arrived(kv.at[kind, at], kv_send.at[kind, at], kv_recv.at[kind, at])

    def rows_wait(slot):
        arrived(qg.at[slot], qg_send.at[0], qg_recv.at[slot])

    def slot_of(first, second):
        return 2 * (other * ORDER.index((second, first)) + core * ORDER.index((first, second))) + core

    rows_sent = iter(range(PEERS))

    def rows_to(slot, there, device):
        send(qg.at[slot], qg.at[there], qg_send.at[next(rows_sent)], qg_recv.at[there], device)

    def second_line(first):
        for k in (3, 1, 2):
            rows_to(slot_of(first, 0), slot_of(first, BACKWARD[k]), lines[1][k])

    def rows_from(first, second):
        slot = slot_of(first, second)
        rows_wait(slot)
        if first and not second:
            second_line(first)
        rows_to(slot, slot, mate)

    for kind in range(2):
        kv_to(kind, 0, 2, up2)
        kv_to(kind, 0, 6, down2)
    for k in (3, 1, 2):
        rows_to(core, slot_of(BACKWARD[k], 0), lines[0][k])
    rows_to(core, core, mate)
    second_line(0)
    for kind in range(2):
        kv_to(kind, 0, 1, up)
        kv_to(kind, 0, 7, down)

    for copy in inputs[6:]:
        copy.wait()
    rows_wait(other)
    own_q = qg[0:2, 0:ROWS].reshape(2 * ROWS, HD)
    own_g = qg[0:2, ROWS : 2 * ROWS].reshape(2 * ROWS, HD)
    block = ck_ref.shape[0]
    cand_token = lax.broadcasted_iota(jnp.int32, (block, 2 * ROWS), 0)
    allowed = (sample_of(cand_token) == sample) & (cand_token <= token)
    score = lax.dot_general(ck_ref[...], own_q, NT, preferred_element_type=F32) * SCORE
    score = jnp.where(allowed, score, NEG)
    own_high = jnp.max(score, axis=0, keepdims=True)
    expon = jnp.exp2(score - own_high)
    product = lax.dot_general(cv_ref[...], own_g, NT, preferred_element_type=F32)
    own_total = jnp.sum(expon, axis=0, keepdims=True)
    own_carry = jnp.sum(expon * product, axis=0, keepdims=True)
    self_e[...] = expon
    self_p[...] = product

    def first_key(place):
        behind = lax.rem(z + NZ - BACK[place], NZ)
        return (((behind * 2 + xh) * 2 + core) * 8 + y * 2 + xl) * KEYS

    starts = [first_key(place).astype(F32) for place in range(NZ)]

    def first_pass(t, groups):
        rows_q = qg[pl.ds(4 * t, 4), 0:ROWS].reshape(TILE, HD)
        rows_g = qg[pl.ds(4 * t, 4), ROWS : 2 * ROWS].reshape(TILE, HD)
        coded = [qg[4 * t + 2 * i, 2 * ROWS : PIECE].astype(F32) for i in range(2)]
        rows_limit = jnp.concatenate([c[0:1] * 256.0 + c[8:9] for c in coded], axis=1)
        for g in groups:
            low, high = GROUPS[g]
            count = (high - low) * KEYS
            keys = kv[0, low:high].reshape(count, HD)
            values = kv[1, low:high].reshape(count, HD)
            score = lax.dot_general(keys, rows_q, NT, preferred_element_type=F32) * SCORE
            index = lax.broadcasted_iota(jnp.int32, (KEYS, TILE), 0).astype(F32)
            masked = []
            for i, place in enumerate(range(low, high)):
                seen = index < rows_limit - starts[place]
                masked.append(jnp.where(seen, score[i * KEYS : (i + 1) * KEYS], NEG))
            score = jnp.concatenate(masked, axis=0)
            top = jnp.max(score, axis=0, keepdims=True)
            expon = jnp.exp2(score - top)
            product = lax.dot_general(values, rows_g, NT, preferred_element_type=F32)
            e_buf[t, low * KEYS : high * KEYS] = expon
            p_buf[t, low * KEYS : high * KEYS] = product
            mg[t, g : g + 1] = top
            tot[t, g : g + 1] = jnp.sum(expon, axis=0, keepdims=True)
            car[t, g : g + 1] = jnp.sum(expon * product, axis=0, keepdims=True)

    def run_first_pass(start, stop, groups):
        def step(t, carry):
            first_pass(t, groups)
            return carry

        lax.fori_loop(start, stop, step, 0)

    def close_rows(t, carry):
        highs = mg[t]
        top = jnp.max(highs, axis=0, keepdims=True)
        weight = jnp.exp2(highs - top)
        total = jnp.sum(tot[t] * weight, axis=0, keepdims=True)
        carried = jnp.sum(car[t] * weight, axis=0, keepdims=True)
        stats = jnp.concatenate([top, total, carried, top], axis=0)
        stat_out[2 * t] = stats[:, : 2 * ROWS]
        stat_out[2 * t + 1] = stats[:, 2 * ROWS :]
        return carry

    def tile_wait(tiles):
        for t in tiles:
            for r in (2 * t, 2 * t + 1):
                if not (isinstance(r, int) and r == 0):
                    rows_wait(2 * r + other)

    for k in (1, 2, 3):
        rows_from(k, 0)
    kv_wait(0, 2)
    kv_to(0, 2, 4, up2)
    kv_to(0, 2, 3, up)
    kv_wait(0, 6)
    kv_to(0, 6, 5, down)
    kv_wait(1, 6)
    kv_to(1, 6, 4, down2)
    kv_to(1, 6, 5, down)
    kv_wait(1, 2)
    kv_to(1, 2, 3, up)
    for k in (1, 2, 3):
        rows_from(0, k)
    for kind in range(2):
        for back in (1, 7):
            kv_wait(kind, back)
    for first, second in ((1, 1), (2, 1), (1, 2), (2, 2)):
        rows_from(first, second)
    tile_wait((0, 1, 2))
    run_first_pass(0, 3, (0, 1))
    for kind in range(2):
        for back in (3, 5, 4):
            kv_wait(kind, back)
    run_first_pass(0, 3, (2,))
    lax.fori_loop(0, 3, close_rows, 0)
    for first, second in ((3, 1), (3, 2), (1, 3), (2, 3), (3, 3)):
        rows_from(first, second)

    def last_tiles(t, carry):
        tile_wait((t,))
        first_pass(t, (0, 1, 2))
        return close_rows(t, carry)

    lax.fori_loop(3, TILES, last_tiles, 0)

    send(stat_out, stat_mate, mate_send, mate_recv, mate)
    for r in FARTHEST:
        slot = 2 * SEEN[r] + core
        send(
            stat_out.at[r], stat_in.at[slot], st_send.at[r], st_recv.at[slot],
            {**chips[r], "core": 1},
        )

    for place in range(NZ):
        kt[:, place * KEYS : (place + 1) * KEYS] = kv[0, place].astype(F32).T.astype(BF16)

    arrived(stat_mate, mate_send, mate_recv)

    def query_products(t, carry):
        pair = [
            jnp.concatenate([ref[2 * t], ref[2 * t + 1]], axis=1) for ref in (stat_out, stat_mate)
        ]
        top = jnp.maximum(pair[0][0:1], pair[1][0:1])
        scaled = [part_of * jnp.exp2(part_of[0:1] - top) for part_of in pair]
        delta = (scaled[0][2:3] + scaled[1][2:3]) / (scaled[0][1:2] + scaled[1][1:2])
        loc[t] = jnp.concatenate([top, delta], axis=0)
        expons, slopes = [], []
        for g, (low, high) in enumerate(GROUPS):
            weight = jnp.exp2(mg[t, g : g + 1] - top)
            expon = e_buf[t, low * KEYS : high * KEYS] * weight
            expons.append(expon.astype(BF16))
            slopes.append((expon * (p_buf[t, low * KEYS : high * KEYS] - delta)).astype(BF16))
        for i, right in enumerate((slopes, expons)):
            ab[t, i] = jnp.dot(kt[...], jnp.concatenate(right, axis=0), preferred_element_type=F32)
        remote(ab.at[t], ab_mate.at[t], ab_send.at[t], ab_recv.at[t], mate).start()
        return carry

    lax.fori_loop(0, TILES, query_products, 0)

    def final_sends():
        copies = []
        for r in FARTHEST:
            for c in (0, 1):
                copies.append(
                    remote(
                        fin_out, fin.at[SEEN[r]], fin_send.at[2 * r + c], fin_recv.at[SEEN[r]],
                        {**chips[r], "core": c},
                    )
                )
        copies.append(remote(fin_out, fin.at[0], fin_send.at[0], fin_recv.at[0], {"core": 0}))
        return copies

    @pl.when(core == 1)
    def _():
        for r in NEAREST:
            for c in range(2):
                arrived(stat_in.at[2 * r + c], st_send.at[1], st_recv.at[2 * r + c])
        stat_in[0] = stat_mate[0]
        stat_in[1] = stat_out[0]
        top = own_high
        for i in range(PEERS):
            top = jnp.maximum(top, stat_in[i][0:1])
        weight = jnp.exp2(own_high - top)
        total, carried = own_total * weight, own_carry * weight
        for i in range(PEERS):
            stats = stat_in[i]
            weight = jnp.exp2(stats[0:1] - top)
            total += stats[1:2] * weight
            carried += stats[2:3] * weight
        inverse = 1.0 / total
        final = jnp.concatenate([top, inverse, carried * inverse, top], axis=0)
        fin_out[...] = final
        fin[0] = final
        for copy in final_sends():
            copy.start()

    @pl.when(core == 0)
    def _():
        arrived(fin.at[0], fin_send.at[0], fin_recv.at[0])

    def final_wait(chips_there):
        for r in chips_there:
            arrived(fin.at[r], fin_send.at[1], fin_recv.at[r])

    def close_weights(t, carry):
        final = jnp.concatenate([fin[2 * t], fin[2 * t + 1]], axis=1)
        mg[t] = jnp.exp2(mg[t] - final[0:1]) * final[1:2]
        return carry


    def second_pass(place, carry, tiles=range(TILES), more=False):
        g = lax.div(place + 1, 3)
        grad_k = jnp.zeros((KEYS, HD), F32)
        grad_v = jnp.zeros((KEYS, HD), F32)
        for t in tiles:
            delta = jnp.concatenate([fin[2 * t, 2:3], fin[2 * t + 1, 2:3]], axis=1)
            at = pl.ds(pl.multiple_of(place * KEYS, KEYS), KEYS)
            probs = e_buf[t, at] * mg[t, pl.ds(g, 1)]
            slopes = (probs * (p_buf[t, at] - delta)).astype(BF16)
            rows_q = qg[4 * t : 4 * t + 4, 0:ROWS].reshape(TILE, HD)
            rows_g = qg[4 * t : 4 * t + 4, ROWS : 2 * ROWS].reshape(TILE, HD)
            grad_v += jnp.dot(probs.astype(BF16), rows_g, preferred_element_type=F32)
            grad_k += jnp.dot(slopes, rows_q, preferred_element_type=F32)
        grad_k = grad_k * SCALING
        part[place, 0] = part[place, 0] + grad_k if more else grad_k
        part[place, 1] = part[place, 1] + grad_v if more else grad_v
        return carry

    def pass_on(kind, back, dst, sem, device, *more):
        at = PLACE[back]
        total = part[at, kind]
        for ref in more:
            total = total + ref[...].astype(F32)
        rs_out[kind, at] = total.astype(BF16)
        send(rs_out.at[kind, at], dst, rs_send.at[kind, at], sem, device)

    near_tiles, far_tiles = range(TILES // 2), range(TILES // 2, TILES)
    final_wait(range(1, CHIPS // 2))
    lax.fori_loop(0, TILES // 2, close_weights, 0)
    lax.fori_loop(0, 3, lambda i, c: second_pass(7 - i, c, near_tiles), 0)
    final_wait(range(CHIPS // 2, CHIPS))
    lax.fori_loop(TILES // 2, TILES, close_weights, 0)
    second_pass(PLACE[4], 0, far_tiles, True)
    pass_on(0, 4, rs_far.at[0], far_recv.at[0], down2)
    pass_on(1, 4, rs_far.at[1], far_recv.at[1], up2)
    second_pass(PLACE[3], 0, far_tiles, True)
    for kind in range(2):
        pass_on(kind, 3, rs_near.at[kind, 0], near_recv.at[kind, 0], down)
    second_pass(PLACE[5], 0, far_tiles, True)
    for kind in range(2):
        pass_on(kind, 5, rs_near.at[kind, 1], near_recv.at[kind, 1], up)

    def query_pass(t, carry):
        final = jnp.concatenate([fin[2 * t], fin[2 * t + 1]], axis=1)
        weight = jnp.exp2(loc[t, 0:1] - final[0:1]) * final[1:2] * SCALING
        slopes, expons = (ab[t, i] + ab_mate[t, i] for i in range(2))
        grads = (slopes - expons * (final[2:3] - loc[t, 1:2])) * weight
        rows = grads.T.astype(BF16)
        for i in range(2):
            for c in range(2):
                at = (2 * i + c) * ROWS
                dq_out[c, 2 * t + i] = rows[at : at + ROWS]
        return carry

    for t in range(TILES):
        remote(ab.at[t], ab_mate.at[t], ab_send.at[t], ab_recv.at[t], mate).wait()
    lax.fori_loop(0, TILES, query_pass, 0)
    for r in FARTHEST:
        send(dq_out.at[core, r], dq_in.at[SEEN[r]], dq_send.at[r], dq_recv.at[SEEN[r]], chips[r])
    lax.fori_loop(0, 2, lambda i, c: second_pass(2 - i, c), 0)
    for kind in range(2):
        pass_on(kind, 7, rs_end.at[kind, 2], end_recv.at[kind, 2], up)
        pass_on(kind, 1, rs_end.at[kind, 0], end_recv.at[kind, 0], down)
    lax.fori_loop(0, 2, lambda i, c: second_pass(4 - i, c), 0)

    def two_on(kind, way):
        arrived(rs_near.at[kind, way], rs_send.at[kind, 0], near_recv.at[kind, way])
        more = [rs_near.at[kind, way]]
        if kind == way:
            arrived(rs_far.at[way], rs_send.at[kind, 0], far_recv.at[way])
            more.append(rs_far.at[way])
        slot = 1 + 2 * way
        device = (down2, up2)[way]
        pass_on(
            kind, (2, 6)[way], rs_end.at[kind, slot], end_recv.at[kind, slot], device, *more
        )

    final = fin[0]
    self_probs = self_e[...] * (jnp.exp2(own_high - final[0:1]) * final[1:2])
    self_slopes = (self_probs * (self_p[...] - final[2:3])).astype(BF16)
    self_keys = ck_ref[...].astype(F32).T.astype(BF16)
    dq_self[...] = (jnp.dot(self_keys, self_slopes, preferred_element_type=F32) * SCALING).T
    for kind, way in ((1, 0), (0, 1), (0, 0), (1, 1)):
        two_on(kind, way)
    second_pass(0, 0)

    grads = dq_self[pl.ds(pl.multiple_of(core * ROWS, ROWS), ROWS)] + dq_out[core, 0].astype(F32)
    for r in NEAREST:
        arrived(dq_in.at[r], dq_send.at[1], dq_recv.at[r])
        grads += dq_in[r].astype(F32)
    gq_ref[...] = jnp.concatenate(
        [grads[h * TOK : (h + 1) * TOK] for h in range(HEADS)], axis=1
    ).astype(BF16)
    for kind, out in enumerate((gk_ref, gv_ref)):
        total = part[0, kind]
        for way in (0, 2, 1, 3):
            arrived(rs_end.at[kind, way], rs_send.at[kind, 0], end_recv.at[kind, way])
            total = total + rs_end[kind, way].astype(F32)
        out[...] = total.astype(BF16)
    for copy in sent:
        copy.wait_send()

    @pl.when(core == 1)
    def _():
        for copy in final_sends():
            copy.wait_send()


def store(*refs):
    sems = refs[6]
    copies = [pltpu.make_async_copy(refs[i], refs[3 + i], sems.at[i]) for i in range(3)]
    for copy in copies:
        copy.start()
    for copy in copies:
        copy.wait()


def body(queries, grad_out, prefix_keys, prefix_values, cand_keys, cand_values, lengths, offsets):
    vmem = pl.BlockSpec(memory_space=pltpu.VMEM)
    anywhere = pl.BlockSpec(memory_space=pl.ANY)
    keys = NZ * KEYS
    block = cand_keys.shape[0]
    sem = pltpu.SemaphoreType.DMA
    found = pl.pallas_call(
        kernel,
        out_shape=(
            pltpu.VMEM(queries.shape, BF16),
            pltpu.VMEM(prefix_keys.shape, BF16),
            pltpu.VMEM(prefix_values.shape, BF16),
        ),
        in_specs=[anywhere] * 8,
        out_specs=(vmem,) * 3,
        scratch_shapes=[
            pltpu.VMEM(queries.shape, BF16),
            pltpu.VMEM(grad_out.shape, BF16),
            pltpu.VMEM(cand_keys.shape, BF16),
            pltpu.VMEM(cand_values.shape, BF16),
            pltpu.SMEM(lengths.shape, jnp.int32),
            pltpu.SMEM(offsets.shape, jnp.int32),
            sem((8,)),
            pltpu.VMEM((PEERS, PIECE, HD), BF16),
            pltpu.VMEM((2, NZ, KEYS, HD), BF16),
            pltpu.VMEM((HD, keys), BF16),
            pltpu.VMEM((TILES, keys, TILE), F32),
            pltpu.VMEM((TILES, keys, TILE), F32),
            pltpu.VMEM((TILES, len(GROUPS), TILE), F32),
            pltpu.VMEM((TILES, len(GROUPS), TILE), F32),
            pltpu.VMEM((TILES, len(GROUPS), TILE), F32),
            pltpu.VMEM((TILES, 2, TILE), F32),
            pltpu.VMEM((TILES, 2, HD, TILE), F32),
            pltpu.VMEM((TILES, 2, HD, TILE), F32),
            pltpu.VMEM((CHIPS, 4, 2 * ROWS), F32),
            pltpu.VMEM((PEERS, 4, 2 * ROWS), F32),
            pltpu.VMEM((CHIPS, 4, 2 * ROWS), F32),
            pltpu.VMEM((4, 2 * ROWS), F32),
            pltpu.VMEM((CHIPS, 4, 2 * ROWS), F32),
            pltpu.VMEM((block, 2 * ROWS), F32),
            pltpu.VMEM((block, 2 * ROWS), F32),
            pltpu.VMEM((2, CHIPS, ROWS, HD), BF16),
            pltpu.VMEM((CHIPS, ROWS, HD), BF16),
            pltpu.VMEM((2 * ROWS, HD), F32),
            pltpu.VMEM((NZ, 2, KEYS, HD), F32),
            pltpu.VMEM((2, NZ, KEYS, HD), BF16),
            pltpu.VMEM((2, 2, KEYS, HD), BF16),
            pltpu.VMEM((2, KEYS, HD), BF16),
            pltpu.VMEM((2, 4, KEYS, HD), BF16),
            sem((PEERS,)),
            sem((PEERS,)),
            sem((2, NZ)),
            sem((2, NZ)),
            sem((CHIPS,)),
            sem((PEERS,)),
            sem((PEERS,)),
            sem((CHIPS,)),
            sem,
            sem,
            sem((TILES,)),
            sem((TILES,)),
            sem((CHIPS,)),
            sem((CHIPS,)),
            sem((2, NZ)),
            sem((2, 2)),
            sem((2,)),
            sem((2, 4)),
        ],
        compiler_params=pltpu.CompilerParams(
            collective_id=0, has_side_effects=True, vmem_limit_bytes=56 * 1024 * 1024
        ),
        name="attention_grads",
    )(queries, grad_out, prefix_keys, prefix_values, cand_keys, cand_values, lengths, offsets)
    return pl.pallas_call(
        store,
        out_shape=tuple(jax.ShapeDtypeStruct(a.shape, BF16) for a in found),
        in_specs=[vmem] * 3,
        out_specs=(anywhere,) * 3,
        scratch_shapes=[sem((3,))],
        name="store",
    )(*(pltpu.with_memory_space_constraint(a, pltpu.VMEM) for a in found))


def solution(mesh):
    torus = Mesh(mesh.devices.reshape(NZ, 2, 2, NY, 2), AXES)
    in_specs = (
        P(CAND_CTX, None),
        P(CAND_CTX, None),
        P(CTX_CAND, None),
        P(CTX_CAND, None),
        P(CAND, None),
        P(CAND, None),
        P(CAND, None),
        P(CAND),
    )
    out_specs = (P(CAND_CTX, None), P(CTX_CAND, None), P(CTX_CAND, None))
    return jax.shard_map(body, mesh=torus, in_specs=in_specs, out_specs=out_specs, check_vma=False)
```
